32 devices in a mesh: row: 2 (over x), col: 4 (over y, core), layer: 4 (over z).
Axes of the slice: x: 2, y: 2, z: 4, core: 2. Of those that a mesh axis runs over, the one named last changes fastest.
Arguments:
- object_field: float32 [2, 512, 1024], P(None, 'row', 'col'), may hold values from -6 to 6
- probe_modes: float32 [2, 4, 256, 256], replicated, may hold values from -6 to 6
- amplitudes: float32 [32, 256, 256], P(('row', 'col', 'layer')), may hold values from 0 to 4
- offsets: int32 [32, 2], P(('row', 'col', 'layer')), may hold values from 0 to 768, as said below
Outputs:
- new_object: float32 [2, 512, 1024], P(None, 'row', 'col')
The draws below stay inside these ranges and needn't reach their ends.
Inputs may be any that keep to these rules, and one draw needn't show every extreme that they name: `offsets`: every patch lies inside the 512 x 1024 object. A position held by the device at tile (r, c) has its corner inside that tile: rows r * 256 to (r + 1) * 256 - 1 and columns c * 256 to (c + 1) * 256 - 1. On a device whose tile row is not the last, its first position's patch reaches into the next tile row.
All inputs are finite; a program needn't handle non-finite values.
Results may differ from the reference program's by a relative error of at most 0.0001.
Values sent between devices are 32-bit elements; how exact they have to be, the bound alone decides.
A program may use at most 64 MiB of HBM per device.

```python
import jax
import jax.numpy as jnp
from jax import lax

PATCH = 256
MODES = 4
TILE_R = 256
TILE_C = 256
POS_DEV = 1
OBJ_R = 512
OBJ_C = 1024
POSITIONS = 32
N_ROW = 2
N_COL = 4
N_LAYER = 4


def draw_offsets(key, part):
    index = jnp.arange(POSITIONS, dtype=jnp.int32)
    device = index // POS_DEV
    slot = index % POS_DEV
    tile_row = device // (N_COL * N_LAYER)
    tile_col = device // N_LAYER % N_COL
    key_rows, key_cols = jax.random.split(jax.random.fold_in(key, 17))
    rows_high = jnp.where(tile_row == N_ROW - 1, TILE_R - PATCH + 1, TILE_R)
    rows_low = jnp.where((slot == 0) & (tile_row < N_ROW - 1), TILE_R - PATCH + 1, 0)
    draw_rows = jax.random.randint(key_rows, (POSITIONS,), 0, 1 << 30, dtype=jnp.int32)
    local_rows = rows_low + draw_rows % (rows_high - rows_low)
    cols_high = jnp.where(tile_col == N_COL - 1, TILE_C - PATCH + 1, TILE_C)
    draw_cols = jax.random.randint(key_cols, (POSITIONS,), 0, 1 << 30, dtype=jnp.int32)
    local_cols = draw_cols % cols_high
    return jnp.stack([tile_row * TILE_R + local_rows, tile_col * TILE_C + local_cols], axis=-1).astype(jnp.int32)


def steps_of(stream_key, shape, cuts, low, top_value):
    level = 1.0
    for axis_at, parts in cuts:
        draws = jax.random.uniform(jax.random.fold_in(jax.random.fold_in(stream_key, 6), axis_at), (parts,), jnp.float32, low / len(cuts), top_value / len(cuts))
        level = level * jnp.repeat(jnp.exp(draws), shape[axis_at] // parts).reshape((-1,) + (1,) * (len(shape) - 1 - axis_at))
    return level


def centred(rng, shape, spread, most, shards=(), kind=jnp.bfloat16):
    entries = jax.random.normal(rng, shape, jnp.float32) * spread
    if len(shards) > 0:
        entries = steps_of(rng, shape, shards, -0.22, 0.18) * entries
    return jnp.clip(entries, min=-most, max=most).astype(kind)


def setup_inputs(seed: int = 0) -> dict:
    seeds = jax.random.split(jax.random.key(seed), 5)
    return {
        "object_field": centred(seeds[0], (2, OBJ_R, OBJ_C), 1.0, 6.0, ((1, 2), (2, 4)), jnp.float32),
        "probe_modes": centred(seeds[1], (2, MODES, PATCH, PATCH), 1.0, 6.0, (), jnp.float32),
        "amplitudes": jnp.clip(4.0 * jax.random.uniform(seeds[2], (POSITIONS, PATCH, PATCH), jnp.float32) ** steps_of(seeds[2], (POSITIONS, PATCH, PATCH), ((0, 32),), -0.2, 0.2), 0.0, 4.0),
        "offsets": draw_offsets(jax.random.fold_in(seeds[4], 71), 0),
    }


SOFTEN = 0.05
DAMPING = 0.5

def reference(object_field, probe_modes, amplitudes, offsets):
    probe = lax.complex(probe_modes[0], probe_modes[1])
    power = lax.optimization_barrier(jnp.sum(probe_modes[0] * probe_modes[0] + probe_modes[1] * probe_modes[1], axis=0))
    zero_index = jnp.int32(0)

    def one_position(index, carry):
        numer, denom = carry
        row_at = offsets[index, 0].astype(jnp.int32)
        col_at = offsets[index, 1].astype(jnp.int32)
        patch = lax.dynamic_slice(object_field, (zero_index, row_at, col_at), (2, PATCH, PATCH))
        exit_wave = probe * lax.complex(patch[0], patch[1])[None]
        far = jnp.fft.fft2(exit_wave, norm='ortho')
        intensity = lax.optimization_barrier(jnp.sum(far.real * far.real + far.imag * far.imag, axis=0))
        ratio = amplitudes[index] / (jnp.sqrt(intensity) + SOFTEN)
        revised = jnp.fft.ifft2(far * ratio[None], norm='ortho')
        contrib = lax.optimization_barrier(jnp.sum(jnp.conj(probe) * revised, axis=0))
        block = jnp.stack([contrib.real, contrib.imag])
        old_block = lax.dynamic_slice(numer, (zero_index, row_at, col_at), (2, PATCH, PATCH))
        numer = lax.dynamic_update_slice(numer, old_block + block, (zero_index, row_at, col_at))
        old_power = lax.dynamic_slice(denom, (row_at, col_at), (PATCH, PATCH))
        denom = lax.dynamic_update_slice(denom, old_power + power, (row_at, col_at))
        return (numer, denom)
    numer0 = jnp.zeros(object_field.shape, jnp.float32)
    denom0 = jnp.zeros(object_field.shape[1:], jnp.float32)
    numer, denom = lax.fori_loop(0, POSITIONS, one_position, (numer0, denom0))
    return (numer + DAMPING * object_field) / (denom + DAMPING)[None]
```

```python
import contextlib
import functools

import jax
import jax.numpy as jnp
import numpy as np
from jax import lax
from jax.experimental import pallas as pl
from jax.experimental.pallas import tpu as pltpu
from jax.sharding import PartitionSpec as P

SOFTEN = 0.05
DAMPING = 0.5
AXES = ("row", "col", "layer")
PARTS = 4
LEAD = 2
IN_ROWS = 32
OUT_ROWS = 16
LAG_IN = 3
LAG_CROSS = 3


def scope(name):
    return contextlib.nullcontext()


def place():
    return tuple(lax.axis_index(a) for a in AXES)


def send(src, dst, send_sem, recv_sem, device):
    return pltpu.make_async_remote_copy(
        src_ref=src,
        dst_ref=dst,
        send_sem=send_sem,
        recv_sem=recv_sem,
        device_id=device,
        device_id_type=pl.DeviceIdType.MESH,
    )


def greet(rows, cols, layers):
    r, c, l = place()
    barrier = pltpu.get_barrier_semaphore()

    def tell(device):
        pl.semaphore_signal(
            barrier, inc=1, device_id=device, device_id_type=pl.DeviceIdType.MESH
        )

    near = (
        (c > 0, (r, c - 1, l)),
        (c < cols - 1, (r, c + 1, l)),
        (r > 0, (r - 1, c, l)),
        (r < rows - 1, (r + 1, c, l)),
    )
    for there, device in near:
        pl.when(there)(functools.partial(tell, device))
    for d in range(1, layers):
        tell((r, c, lax.rem(l + d, layers)))
    count = layers - 1
    for there, _ in near:
        count += there.astype(jnp.int32)
    pl.semaphore_wait(barrier, count)


def split(x):
    high = x.astype(jnp.bfloat16)
    return high, (x - high.astype(jnp.float32)).astype(jnp.bfloat16)


def prod(left, right):
    def one(a, b):
        return jnp.dot(a, b, preferred_element_type=jnp.float32)

    return one(left[0], right[0]) + (one(left[0], right[1]) + one(left[1], right[0]))


def corner_of(offs, group, layer, side):
    r, c, _ = place()
    tile_row = r - (1 if group >= 2 else 0)
    tile_col = c - (group % 2)
    return offs[group, layer, 0, 0] - tile_row * side, offs[group, layer, 0, 1] - tile_col * side


def kernel(
    sizes,
    corner_hbm, obj_hbm, probe_hbm, amp_hbm, fwd_high_hbm, fwd_low_hbm, inv_high_hbm, inv_low_hbm,
    out,
    corner, obj, probe, amp, fwd_high, fwd_low, inv_high, inv_low, offs, corners,
    right, below, diag, rolled, lines, far, ratio, power, weight,
    terms, left, own, lower, upper, inbound, crossed,
    s_load, s_corner, s_off, r_off, s_pass, r_pass,
    s_right, r_right, s_below, r_below, s_share, r_share, s_diag, r_diag, s_diag2, r_diag2,
    s_left, r_left, s_down, r_down, s_in, r_in, s_cross, r_cross, s_res, r_res,
):
    rows, cols, layers = sizes
    side = obj.shape[1]
    modes = probe.shape[1]
    tall = side // PARTS
    pieces_in = side // IN_ROWS
    steps = side // OUT_ROWS
    r, c, l = place()
    has_right, has_left = c < cols - 1, c > 0
    has_below, has_above = r < rows - 1, r > 0
    half = layers // 2
    low_half = l < half
    is_hub = (l == half - 1) | (l == half)
    has_outer = (l > 0) & (l < layers - 1)
    inner = (r, c, l + jnp.where(low_half, 1, -1))
    outer = (r, c, l + jnp.where(low_half, -1, 1))
    odd = lax.rem(l, 2)
    partner = (r, c, l + 1 - 2 * odd)
    west, east = (r, c - 1, l), (r, c + 1, l)
    north, south = (r - 1, c, l), (r + 1, c, l)

    loads = [
        pltpu.make_async_copy(src, dst, s_load.at[i])
        for i, (src, dst) in enumerate(
            (
                (corner_hbm, corner),
                (obj_hbm, obj),
                (probe_hbm, probe),
                (fwd_high_hbm, fwd_high),
                (fwd_low_hbm, fwd_low),
                (amp_hbm, amp),
                (inv_high_hbm, inv_high),
                (inv_low_hbm, inv_low),
            )
        )
    ]
    for copy in loads:
        copy.start()
    with scope("greet"):
        greet(rows, cols, layers)
    with scope("load"):
        loads[1].wait()

    def chunk(k, size):
        return pl.ds(k * size, size)

    lefts = [
        send(
            obj.at[:, chunk(k, IN_ROWS)], right.at[:, chunk(k, IN_ROWS)],
            s_right.at[k], r_right.at[k], west,
        )
        for k in range(pieces_in)
    ]
    ups, shares, diags, diags2 = [], [], [], []
    for i in range(pieces_in // 2):
        mine, other = chunk(2 * i + odd, IN_ROWS), chunk(2 * i + 1 - odd, IN_ROWS)
        ups.append(send(obj.at[:, mine], below.at[:, mine], s_below.at[i], r_below.at[i], north))
        shares.append(
            send(below.at[:, mine], below.at[:, mine], s_share.at[i], r_share.at[i], partner)
        )
        diags.append(send(below.at[:, mine], diag.at[:, mine], s_diag.at[i], r_diag.at[i], west))
        diags2.append(
            send(below.at[:, other], diag.at[:, other], s_diag2.at[i], r_diag2.at[i], west)
        )
    for i in range(pieces_in // 2):
        pl.when(has_above)(ups[i].start)
    for k in range(pieces_in):
        pl.when(has_left)(lefts[k].start)
    loads[0].wait()
    at = lax.broadcasted_iota(jnp.int32, (1, 1, 128), 2)
    offs[0, pl.ds(l, 1)] = jnp.where(at == 0, corner[0, 0], corner[0, 1])
    mine = offs.at[0, pl.ds(l, 1)]
    around = [(d, lax.rem(l + d, layers)) for d in range(1, layers)]
    peers = [send(mine, mine, s_off.at[d], r_off.at[d], (r, c, p)) for d, p in around]
    for peer in peers:
        peer.start()
    down = corner[0, 0] - r * side
    over = corner[0, 1] - c * side
    loads[2].wait()

    def prepare(m):
        for h in range(2):
            rolled[h, m] = pltpu.roll(pltpu.roll(probe[h, m], down, 0), over, 1)

    def forward(i):
        @pl.when(has_below)
        def _():
            ups[i].wait_recv()
            shares[i].start()
            pl.when(has_left)(diags[i].start)

    def forward2(i):
        @pl.when(has_below)
        def _():
            shares[i].wait_recv()
            pl.when(has_left)(diags2[i].start)

    across = send(offs.at[0], offs.at[1], s_pass.at[0], r_pass.at[0], east)
    down0 = send(offs.at[0], offs.at[2], s_pass.at[1], r_pass.at[1], south)
    down1 = send(offs.at[1], offs.at[3], s_pass.at[2], r_pass.at[2], south)

    def weigh(groups):
        there = (None, has_left, has_above, has_left & has_above)
        wide = lax.broadcasted_iota(jnp.int32, (side, side), 1)
        deep = lax.broadcasted_iota(jnp.int32, (side, side), 0)
        for group in groups:

            def add(layer, carry, group=group):
                a, b = corner_of(corners, group, layer, side)
                window = pltpu.roll(pltpu.roll(power[...], a, 0), b, 1)
                keep = (deep < a) if group >= 2 else (deep >= a)
                keep &= (wide < b) if group % 2 else (wide >= b)
                weight[...] += jnp.where(keep, window, 0.0)
                return carry

            def all_layers(add=add):
                lax.fori_loop(0, layers, add, 0)

            if there[group] is None:
                all_layers()
            else:
                pl.when(there[group])(all_layers)

    def fetch():
        copy = pltpu.make_async_copy(offs, corners, s_corner)
        copy.start()
        copy.wait()

    with scope("prep0"):
        prepare(0)
    with scope("peers"):
        for peer in peers:
            peer.wait()
        pl.when(has_right)(across.start)
    with scope("prep1"):
        power[...] = jnp.zeros_like(power)
        for m in range(1, modes):
            prepare(m)
        for m in range(modes):
            power[...] += probe[0, m] * probe[0, m] + probe[1, m] * probe[1, m]
    with scope("fwd0"):
        forward(0)
    with scope("across"):
        pl.when(has_left)(across.wait_recv)

        @pl.when(jnp.logical_not(has_left))
        def _():
            offs[1] = jnp.zeros(offs.shape[1:], jnp.int32)

        @pl.when(has_below)
        def _():
            down0.start()
            pl.when(has_left)(down1.start)

    weight[...] = jnp.full_like(weight, DAMPING)
    for i in range(1, pieces_in // 2 + 1):
        with scope(f"fwd{i}"):
            if i < pieces_in // 2:
                forward(i)
            forward2(i - 1)
        if i == 1:

            @pl.when(jnp.logical_not(has_above))
            def _():
                with scope("fetch"):
                    offs[2] = jnp.zeros(offs.shape[1:], jnp.int32)
                    offs[3] = jnp.zeros(offs.shape[1:], jnp.int32)
                    fetch()

        if i in (2, 3):

            @pl.when(jnp.logical_not(has_above))
            def _(i=i):
                with scope("weight"):
                    weigh((i - 2,))

    @pl.when(jnp.logical_not(has_above))
    def _():
        weight[...] = 1.0 / weight[...]

    with scope("loads"):
        for copy in loads[3:]:
            copy.wait()
    fwd, inv = (fwd_high, fwd_low), (inv_high, inv_low)

    def last(x, table):
        return prod(split(x), (table[0][...], table[1][...]))

    def first(table, x):
        a = (table[0][:, :side], table[1][:, :side])
        b = (table[0][:, side:], table[1][:, side:])
        return prod(a, split(x[:, :side])) + prod(b, split(x[:, side:]))

    lane = lax.broadcasted_iota(jnp.int32, (tall, side), 1)
    line = lax.broadcasted_iota(jnp.int32, (tall, side), 0)
    per_part = tall // IN_ROWS

    for k in range(PARTS):
        part = chunk(k, tall)
        with scope(f"merge{k}"):
            high = line + k * tall < down
            for h in range(2):
                own[h, part] = obj[h, part]

            @pl.when(has_right)
            def _():
                for i in range(k * per_part, (k + 1) * per_part):
                    lefts[i].wait_recv()
                for h in range(2):
                    own[h, part] = jnp.where(lane < over, right[h, part], own[h, part])

            @pl.when(has_below)
            def _():
                for h in range(2):
                    own[h, part] = jnp.where(high & (lane >= over), below[h, part], own[h, part])

            @pl.when(has_below & has_right)
            def _():
                for i in range(k * per_part // 2, (k + 1) * per_part // 2):
                    diags[i].wait_recv()
                    diags2[i].wait_recv()
                for h in range(2):
                    own[h, part] = jnp.where(high & (lane < over), diag[h, part], own[h, part])

        with scope(f"first{k}"):
            patch = [own[h, part] for h in range(2)]
            waves = []
            for m in range(modes):
                real, imag = (rolled[h, m, part] for h in range(2))
                waves.append(
                    jnp.concatenate(
                        [real * patch[0] - imag * patch[1], real * patch[1] + imag * patch[0]],
                        axis=1,
                    )
                )
            spread = last(jnp.concatenate(waves, axis=0), fwd)
            for m in range(modes):
                lines[m, part] = spread[m * tall : (m + 1) * tall]

    ratio[...] = jnp.zeros_like(ratio)

    def columns(m, carry):
        spread = first(inv, lines[m])
        far[m] = spread
        ratio[...] += spread[:side] * spread[:side] + spread[side:] * spread[side:]
        return carry

    with scope("columns"):
        lax.fori_loop(0, modes, columns, 0)
    ratio[...] = amp[0] / (jnp.sqrt(ratio[...]) + SOFTEN)

    def back(m, carry):
        scale = ratio[...]
        fixed = jnp.concatenate([far[m, :side] * scale, far[m, side:] * scale], axis=1)
        x = first(fwd, fixed)
        lines[m] = jnp.concatenate([x[:side], x[side:]], axis=1)
        return carry

    with scope("back"):
        lax.fori_loop(0, modes, back, 0)

    @pl.when(has_above)
    def _():
        with scope("fetch"):
            down0.wait_recv()
            pl.when(has_left)(down1.wait_recv)

            @pl.when(jnp.logical_not(has_left))
            def _():
                offs[3] = jnp.zeros(offs.shape[1:], jnp.int32)

            fetch()

    left_down, left_over = corner_of(corners, 1, l, side)

    def flow(src, dst, sems, device):
        return [
            send(
                src.at[:, chunk(k, OUT_ROWS)], dst.at[:, chunk(k, OUT_ROWS)],
                sems[0].at[k], sems[1].at[k], device,
            )
            for k in range(steps)
        ]

    rights = flow(terms, left, (s_left, r_left), east)
    downs = flow(lower, upper, (s_down, r_down), south)
    inward = flow(own, inbound, (s_in, r_in), inner)
    swaps = flow(own, crossed, (s_cross, r_cross), inner)
    results = flow(out, out, (s_res, r_res), outer)
    per_tall = tall // OUT_ROWS

    def rows_back(k):
        part = chunk(k, tall)
        x = jnp.concatenate([lines[m, part] for m in range(modes)], axis=0)
        x = last(x, inv)
        sums = [jnp.zeros((tall, side), jnp.float32)] * 2
        for m in range(modes):
            new_real = x[m * tall : (m + 1) * tall, :side]
            new_imag = x[m * tall : (m + 1) * tall, side:]
            real, imag = (rolled[h, m, part] for h in range(2))
            sums[0] += real * new_real + imag * new_imag
            sums[1] += real * new_imag - imag * new_real
        for h in range(2):
            terms[h, part] = sums[h]

        @pl.when(has_right)
        def _():
            for j in range(k * per_tall, (k + 1) * per_tall):
                rights[j].start()

    thin_lane = lax.broadcasted_iota(jnp.int32, (OUT_ROWS, side), 1)
    thin_line = lax.broadcasted_iota(jnp.int32, (OUT_ROWS, side), 0)

    def share_out(j):
        part = chunk(j, OUT_ROWS)
        at = thin_line + j * OUT_ROWS
        for h in range(2):
            mine = jnp.where(thin_lane >= over, terms[h, part], 0.0)
            own[h, part] = jnp.where(at >= down, mine, 0.0)
            lower[h, part] = jnp.where(at < down, mine, 0.0)

        @pl.when(has_left)
        def _():
            rights[j].wait_recv()
            for h in range(2):
                other = jnp.where(thin_lane < left_over, left[h, part], 0.0)
                own[h, part] += jnp.where(at >= left_down, other, 0.0)
                lower[h, part] += jnp.where(at < left_down, other, 0.0)

        pl.when(has_below)(downs[j].start)

    def enter(j):
        @pl.when(jnp.logical_not(has_outer))
        def _():
            if layers == 2:
                swaps[j].start()
            else:
                inward[j].start()

    def gather(j):
        part = chunk(j, OUT_ROWS)

        @pl.when(has_outer)
        def _():
            inward[j].wait_recv()
            for h in range(2):
                own[h, part] += inbound[h, part]
            pl.when(is_hub)(swaps[j].start)
            pl.when(jnp.logical_not(is_hub))(inward[j].start)

    def finish(j):
        part = chunk(j, OUT_ROWS)

        @pl.when(is_hub)
        def _():
            swaps[j].wait_recv()
            for h in range(2):
                number = own[h, part] + crossed[h, part] + DAMPING * obj[h, part]
                out[h, part] = number * weight[part]
            pl.when(has_outer)(results[j].start)

    def chain(s):
        if s < steps:
            enter(s)
        if LAG_IN <= s < steps + LAG_IN:
            gather(s - LAG_IN)
        if s >= LAG_IN + LAG_CROSS:
            finish(s - LAG_IN - LAG_CROSS)

    span = steps + LAG_IN + LAG_CROSS
    for k in range(LEAD):
        with scope(f"rb{k}"):
            rows_back(k)
    for s in range(span):
        if s % per_tall == 0 and s // per_tall + LEAD < PARTS:
            with scope(f"rb{s // per_tall + LEAD}"):
                rows_back(s // per_tall + LEAD)
        with scope(f"out{s}"):
            if s < steps:
                share_out(s)
            pl.when(jnp.logical_not(has_above))(functools.partial(chain, s))

    @pl.when(has_above)
    def _():
        with scope("weight"):
            weigh(range(4))
            weight[...] = 1.0 / weight[...]
        for s in range(span):
            with scope(f"chain{s}"):
                if s < steps:
                    part = chunk(s, OUT_ROWS)
                    downs[s].wait_recv()
                    for h in range(2):
                        own[h, part] += upper[h, part]
                chain(s)

    @pl.when(jnp.logical_not(is_hub))
    def _():
        for j in range(steps):
            with scope(f"res{j}"):
                results[j].wait_recv()
                pl.when(has_outer)(results[j].start)

    def sent(there, copies):
        @pl.when(there)
        def _():
            for copy in copies:
                copy.wait_send()

    with scope("drain"):
        sent(has_left, lefts)
        sent(has_above, ups)
        sent(has_below, shares + [down0])
        sent(has_below & has_left, diags + diags2 + [down1])
        sent(has_right, rights + [across])
        sent(has_below, downs)
        sent(jnp.logical_not(is_hub), inward)
        sent(is_hub, swaps)
        sent(has_outer, results)


def tables(side):
    steps = np.arange(side)
    angle = (steps[:, None] * steps[None, :] % side) * (2.0 * np.pi / side)
    real, imag = np.cos(angle) / np.sqrt(side), -np.sin(angle) / np.sqrt(side)
    both = np.block([[real, imag], [-imag, real]])

    def halves(x):
        x = x.astype(np.float32)
        high = x.astype(jnp.bfloat16)
        return high, (x - high.astype(np.float32)).astype(jnp.bfloat16)

    return halves(both) + halves(both.T)


def body(sizes, object_field, probe_modes, amplitudes, offsets):
    rows, cols, layers = sizes
    side = object_field.shape[1]
    assert object_field.shape[2] == side and probe_modes.shape[2] == side
    assert offsets.shape[0] == 1 and layers % 2 == 0
    assert side % (PARTS * 2 * IN_ROWS) == 0 and side % (PARTS * OUT_ROWS) == 0
    modes = probe_modes.shape[1]
    hbm = pl.BlockSpec(memory_space=pltpu.MemorySpace.HBM)
    vmem = pl.BlockSpec(memory_space=pltpu.MemorySpace.VMEM)
    pair = (2, side, side)
    f32 = jnp.float32
    dma = pltpu.SemaphoreType.DMA
    tabs = tuple(jnp.asarray(t) for t in tables(side))
    tab = pltpu.VMEM((2 * side, 2 * side), jnp.bfloat16)
    plane = pltpu.VMEM((side, side), f32)
    whole = pltpu.VMEM(pair, f32)
    corners = (4, layers, 1, 128)
    pieces_in, steps = side // IN_ROWS, side // OUT_ROWS
    return pl.pallas_call(
        functools.partial(kernel, sizes),
        out_shape=pltpu.VMEM(pair, f32),
        in_specs=[hbm] * 8,
        out_specs=vmem,
        scratch_shapes=[
            pltpu.SMEM((1, 2), jnp.int32),
            whole,
            pltpu.VMEM(probe_modes.shape, f32),
            pltpu.VMEM((1, side, side), f32),
        ]
        + [tab] * 4
        + [pltpu.VMEM(corners, jnp.int32), pltpu.SMEM(corners, jnp.int32)]
        + [whole] * 3
        + [
            pltpu.VMEM(probe_modes.shape, f32),
            pltpu.VMEM((modes, side, 2 * side), f32),
            pltpu.VMEM((modes, 2 * side, side), f32),
        ]
        + [plane] * 3
        + [whole] * 7
        + [dma((8,)), dma(())]
        + [dma((layers,))] * 2
        + [dma((3,))] * 2
        + [dma((pieces_in,))] * 2
        + [dma((pieces_in // 2,))] * 8
        + [dma((steps,))] * 10,
        compiler_params=pltpu.CompilerParams(
            collective_id=0, has_side_effects=True, vmem_limit_bytes=58 * 1024 * 1024
        ),
        name="update",
    )(offsets, object_field, probe_modes, amplitudes, *tabs)


def solution(mesh):
    sizes = tuple(mesh.shape[a] for a in AXES)
    placed = (
        P(None, "row", "col"),
        P(),
        P(("row", "col", "layer"), None, None),
        P(("row", "col", "layer"), None),
    )
    return jax.shard_map(
        functools.partial(body, sizes),
        mesh=mesh,
        in_specs=placed,
        out_specs=P(None, "row", "col"),
        check_vma=False,
    )
```

```python
import contextlib
import functools

import jax
import jax.numpy as jnp
import numpy as np
from jax import lax
from jax.experimental import pallas as pl
from jax.experimental.pallas import tpu as pltpu
from jax.sharding import PartitionSpec as P

SOFTEN = 0.05
DAMPING = 0.5
AXES = ("row", "col", "layer")
PARTS = 4
IN_ROWS = 16
UNROLL = 4
OUT_ROWS = 16
LAG_IN = 3
LAG_CROSS = 3


def scope(name):
    return contextlib.nullcontext()


def place():
    return tuple(lax.axis_index(a) for a in AXES)


def send(src, dst, send_sem, recv_sem, device):
    return pltpu.make_async_remote_copy(
        src_ref=src,
        dst_ref=dst,
        send_sem=send_sem,
        recv_sem=recv_sem,
        device_id=device,
        device_id_type=pl.DeviceIdType.MESH,
    )


def greet(rows, cols, layers):
    r, c, l = place()
    barrier = pltpu.get_barrier_semaphore()

    def tell(device):
        pl.semaphore_signal(
            barrier, inc=1, device_id=device, device_id_type=pl.DeviceIdType.MESH
        )

    near = (
        (c > 0, (r, c - 1, l)),
        (c < cols - 1, (r, c + 1, l)),
        (r > 0, (r - 1, c, l)),
        (r < rows - 1, (r + 1, c, l)),
    )
    for there, device in near:
        pl.when(there)(functools.partial(tell, device))
    for d in range(1, layers):
        tell((r, c, lax.rem(l + d, layers)))
    count = layers - 1
    for there, _ in near:
        count += there.astype(jnp.int32)
    pl.semaphore_wait(barrier, count)


def split(x):
    high = x.astype(jnp.bfloat16)
    return high, (x - high.astype(jnp.float32)).astype(jnp.bfloat16)


def prod(left, right):
    def one(a, b):
        return jnp.dot(a, b, preferred_element_type=jnp.float32)

    return one(left[0], right[0]) + (one(left[0], right[1]) + one(left[1], right[0]))


def corner_of(offs, group, layer, side):
    r, c, _ = place()
    tile_row = r - (1 if group >= 2 else 0)
    tile_col = c - (group % 2)
    return offs[group, layer, 0, 0] - tile_row * side, offs[group, layer, 0, 1] - tile_col * side


def kernel(
    sizes,
    corner_hbm, obj_hbm, probe_hbm, amp_hbm, fwd_high_hbm, fwd_low_hbm, inv_high_hbm, inv_low_hbm,
    out,
    corner, obj, probe, amp, fwd_high, fwd_low, inv_high, inv_low, offs, corners,
    right, below, diag, rolled, lines, far, ratio, power, weight,
    terms, left, own, lower, upper, inbound, crossed,
    s_load, s_corner, s_send, r_off, r_pass,
    r_right, r_below, r_share, r_diag, r_diag2, r_left, r_down, r_in, r_last,
):
    rows, cols, layers = sizes
    side = obj.shape[1]
    mid = side // 2
    modes = probe.shape[1]
    tall = side // PARTS
    pieces = side // IN_ROWS // 2
    steps = side // OUT_ROWS
    r, c, l = place()
    has_right, has_left = c < cols - 1, c > 0
    has_below, has_above = r < rows - 1, r > 0
    half = layers // 2
    low_half = l < half
    is_hub = (l == half - 1) | (l == half)
    has_outer = (l > 0) & (l < layers - 1)
    inner = (r, c, l + jnp.where(low_half, 1, -1))
    outer = (r, c, l + jnp.where(low_half, -1, 1))
    odd = lax.rem(l, 2)
    partner = (r, c, l + 1 - 2 * odd)
    west, east = (r, c - 1, l), (r, c + 1, l)
    north, south = (r - 1, c, l), (r + 1, c, l)
    odd_col = lax.rem(c, 2) == 1

    loads = [
        pltpu.make_async_copy(src, dst, s_load.at[i])
        for i, (src, dst) in enumerate(
            (
                (corner_hbm, corner),
                (obj_hbm, obj),
                (probe_hbm, probe),
                (amp_hbm, amp),
                (fwd_high_hbm, fwd_high),
                (fwd_low_hbm, fwd_low),
                (inv_high_hbm, inv_high),
                (inv_low_hbm, inv_low),
            )
        )
    ]
    for copy in loads:
        copy.start()
    with scope("greet"):
        greet(rows, cols, layers)
    with scope("load"):
        loads[1].wait()

    def chunk(k, size):
        return pl.ds(k * size, size)

    def piece(src, dst, part, send_sem, recv_sem, device):
        return send(src.at[:, part], dst.at[:, part], s_send.at[send_sem], recv_sem, device)

    lefts, lefts2, ups, shares, diags, diags2, extras = [], [], [], [], [], [], []
    for i in range(pieces):
        mine, other = chunk(2 * i + odd, IN_ROWS), chunk(2 * i + 1 - odd, IN_ROWS)
        lefts.append(piece(obj, right, mine, 0, r_right.at[i], west))
        lefts2.append(piece(obj, right, other, 0, r_right.at[pieces + i], west))
        ups.append(piece(obj, below, mine, 1, r_below.at[i], north))
        shares.append(piece(below, below, mine, 2, r_share.at[i], partner))
        diags.append(piece(below, diag, mine, 3, r_diag.at[i], west))
        diags2.append(piece(below, diag, other, 4, r_diag2.at[i], west))
        extras.append(piece(right, diag, other, 5, r_diag2.at[i], north))
    for copy in ups:
        pl.when(has_above)(copy.start)
    for copy in lefts2 + lefts:
        pl.when(has_left)(copy.start)
    with scope("load0"):
        loads[0].wait()
    at = lax.broadcasted_iota(jnp.int32, (1, 1, 128), 2)
    offs[0, pl.ds(l, 1)] = jnp.where(at == 0, corner[0, 0], corner[0, 1])
    mine = offs.at[0, pl.ds(l, 1)]
    around = [(d, lax.rem(l + d, layers)) for d in range(1, layers)]
    peers = [send(mine, mine, s_send.at[6], r_off.at[d - 1], (r, c, p)) for d, p in around]
    for peer in peers:
        peer.start()
    down = corner[0, 0] - r * side
    over = corner[0, 1] - c * side
    with scope("load2"):
        loads[2].wait()

    def prepare(m):
        for h in range(2):
            rolled[h, m] = pltpu.roll(pltpu.roll(probe[h, m], down, 0), over, 1)

    def forward(i):
        @pl.when(has_below)
        def _():
            ups[i].wait_recv()
            shares[i].start()
            pl.when(has_left)(diags[i].start)

        @pl.when(has_above & has_right & odd_col)
        def _():
            lefts2[i].wait_recv()
            extras[i].start()

    def forward2(i):
        @pl.when(has_below)
        def _():
            shares[i].wait_recv()
            pl.when(has_left & odd_col)(diags2[i].start)

    across = send(offs.at[0], offs.at[1], s_send.at[7], r_pass.at[0], east)
    down0 = send(offs.at[0], offs.at[2], s_send.at[8], r_pass.at[1], south)
    down1 = send(offs.at[1], offs.at[3], s_send.at[9], r_pass.at[2], south)

    def weigh(groups, first=0, last=layers):
        there = (None, has_left, has_above, has_left & has_above)
        wide = lax.broadcasted_iota(jnp.int32, (side, side), 1)
        deep = lax.broadcasted_iota(jnp.int32, (side, side), 0)
        for group in groups:

            def add(layer, carry, group=group):
                a, b = corner_of(corners, group, layer, side)
                window = pltpu.roll(pltpu.roll(power[...], a, 0), b, 1)
                keep = (deep < a) if group >= 2 else (deep >= a)
                keep &= (wide < b) if group % 2 else (wide >= b)
                weight[...] += jnp.where(keep, window, 0.0)
                return carry

            def all_layers(add=add):
                lax.fori_loop(first, last, add, 0)

            if there[group] is None:
                all_layers()
            else:
                pl.when(there[group])(all_layers)

    def fetch():
        copy = pltpu.make_async_copy(offs, corners, s_corner)
        copy.start()
        copy.wait()

    fetched = pltpu.make_async_copy(offs, corners, s_corner)

    with scope("prep"):
        for m in range(modes):
            prepare(m)
    with scope("amp"):
        power[...] = jnp.zeros_like(power)
        for m in range(modes):
            power[...] += probe[0, m] * probe[0, m] + probe[1, m] * probe[1, m]
        loads[3].wait()
        wide = lax.broadcasted_iota(jnp.int32, (side, side), 1)
        deep = lax.broadcasted_iota(jnp.int32, (side, side), 0)

        def pick(to, start):
            return to == jnp.where(start < mid, 2 * start, 2 * start - side + 1)

        turn = jnp.where(pick(wide, deep), 1.0, 0.0).astype(jnp.bfloat16)
        back_turn = jnp.where(pick(deep, wide), 1.0, 0.0).astype(jnp.bfloat16)

        def moved(x, along):
            total = None
            for _ in range(3):
                high = x.astype(jnp.bfloat16)
                x = x - high.astype(jnp.float32)
                pair = (turn, high) if along == 0 else (high, back_turn)
                one = jnp.dot(*pair, preferred_element_type=jnp.float32)
                total = one if total is None else total + one
            return total

        amp[0] = moved(moved(amp[0], 0), 1)
        weight[...] = jnp.full_like(weight, DAMPING)

    with scope("peers"):
        for peer in peers:
            peer.wait_recv()
        pl.when(has_right)(across.start)
    with scope("fwd0"):
        forward(0)
    for i in (1, 2):
        with scope(f"fwd{i}"):
            forward(i)
    with scope("across"):

        @pl.when(has_left)
        def _():
            across.wait_recv()

        @pl.when(jnp.logical_not(has_left))
        def _():
            offs[1] = jnp.zeros(offs.shape[1:], jnp.int32)

        @pl.when(has_below)
        def _():
            down0.start()
            pl.when(has_left)(down1.start)

        @pl.when(jnp.logical_not(has_above))
        def _():
            offs[2] = jnp.zeros(offs.shape[1:], jnp.int32)
            offs[3] = jnp.zeros(offs.shape[1:], jnp.int32)
            fetched.start()

    quarters = [(g, q * layers // 2, (q + 1) * layers // 2) for g in (0, 1) for q in range(2)]
    for i in range(3, pieces + 4):
        with scope(f"fwd{i}"):
            if i < pieces:
                forward(i)
            if i >= 4:
                forward2(i - 4)
        if 3 < i < 8:

            @pl.when(jnp.logical_not(has_above) & is_hub)
            def _(i=i):
                with scope(f"weight{i}"):
                    if i == 4:
                        fetched.wait()
                    group, start, stop = quarters[i - 4]
                    weigh((group,), start, stop)

    pl.when(jnp.logical_not(has_above | is_hub))(fetched.wait)

    with scope("loads"):
        for copy in loads[4:]:
            copy.wait()
    fwd, inv = (fwd_high, fwd_low), (inv_high, inv_low)

    def after(x, table, which):
        return prod(split(x), (table[0][which], table[1][which]))

    def ahead(table, which, x):
        return prod((table[0][which], table[1][which]), split(x))

    lane = lax.broadcasted_iota(jnp.int32, (tall, side), 1)
    line = lax.broadcasted_iota(jnp.int32, (tall, side), 0)
    per_part_in = tall // IN_ROWS // 2

    for k in range(PARTS):
        part = chunk(k, tall)
        with scope(f"merge{k}"):
            high = line + k * tall < down
            for h in range(2):
                own[h, part] = obj[h, part]

            @pl.when(has_right & jnp.logical_not(has_above & odd_col))
            def _():
                for i in range(k * per_part_in, (k + 1) * per_part_in):
                    lefts2[i].wait_recv()

            @pl.when(has_right)
            def _():
                for i in range(k * per_part_in, (k + 1) * per_part_in):
                    lefts[i].wait_recv()
                for h in range(2):
                    own[h, part] = jnp.where(lane < over, right[h, part], own[h, part])

            @pl.when(has_below)
            def _():
                for h in range(2):
                    own[h, part] = jnp.where(high & (lane >= over), below[h, part], own[h, part])

            @pl.when(has_below & has_right)
            def _():
                for i in range(k * per_part_in, (k + 1) * per_part_in):
                    diags[i].wait_recv()
                    diags2[i].wait_recv()
                for h in range(2):
                    own[h, part] = jnp.where(high & (lane < over), diag[h, part], own[h, part])

        with scope(f"first{k}"):
            patch = [own[h, part] for h in range(2)]
            sums, gaps = [], []
            for m in range(modes):
                real, imag = (rolled[h, m, part] for h in range(2))
                new = (real * patch[0] - imag * patch[1], real * patch[1] + imag * patch[0])
                sums.append(jnp.concatenate([x[:, :mid] + x[:, mid:] for x in new], axis=1))
                gaps.append(jnp.concatenate([x[:, :mid] - x[:, mid:] for x in new], axis=1))
            even = after(jnp.concatenate(sums, axis=0), fwd, 0)
            uneven = after(jnp.concatenate(gaps, axis=0), fwd, 1)
            for m in range(modes):
                here = slice(m * tall, (m + 1) * tall)
                for h in range(2):
                    there = slice(h * mid, (h + 1) * mid)
                    lines[m, h, part] = jnp.concatenate(
                        [even[here, there], uneven[here, there]], axis=1
                    )

    ratio[...] = jnp.zeros_like(ratio)

    def columns(m, carry):
        x = [lines[m, h] for h in range(2)]
        sums = jnp.concatenate([p[:mid] + p[mid:] for p in x], axis=0)
        gaps = jnp.concatenate([p[:mid] - p[mid:] for p in x], axis=0)
        for which, y in enumerate((sums, gaps)):
            spread = ahead(inv, which, y)
            far[m, which] = spread
            here = slice(which * mid, (which + 1) * mid)
            ratio[here] += spread[:mid] * spread[:mid] + spread[mid:] * spread[mid:]
        return carry

    with scope("columns"):
        lax.fori_loop(0, modes, columns, 0, unroll=UNROLL)
    ratio[...] = amp[0] / (jnp.sqrt(ratio[...]) + SOFTEN)

    def back(m, carry):
        turned = []
        for which in range(2):
            scale = ratio[which * mid : (which + 1) * mid]
            fixed = jnp.concatenate([far[m, which, :mid] * scale, far[m, which, mid:] * scale], axis=0)
            turned.append(ahead(fwd, which, fixed))
        total, gap = turned[0] + turned[1], turned[0] - turned[1]
        for h in range(2):
            there = slice(h * mid, (h + 1) * mid)
            lines[m, h, :mid] = total[there]
            lines[m, h, mid:] = gap[there]
        return carry

    with scope("back"):
        lax.fori_loop(0, modes, back, 0, unroll=UNROLL)

    @pl.when(has_above)
    def _():
        with scope("fetch"):
            down0.wait_recv()
            pl.when(has_left)(down1.wait_recv)

            @pl.when(jnp.logical_not(has_left))
            def _():
                offs[3] = jnp.zeros(offs.shape[1:], jnp.int32)

            fetched.start()
            fetched.wait()

    left_down, left_over = corner_of(corners, 1, l, side)

    def flow(src, dst, send_sem, recv_sem, device):
        return [
            piece(src, dst, chunk(k, OUT_ROWS), send_sem, recv_sem.at[k], device)
            for k in range(steps)
        ]

    rights = flow(terms, left, 10, r_left, east)
    downs = flow(lower, upper, 11, r_down, south)
    inward = flow(own, inbound, 12, r_in, inner)
    swaps = flow(own, crossed, 13, r_last, inner)
    results = flow(out, out, 14, r_last, outer)
    per_tall = tall // OUT_ROWS

    def rows_back(k):
        part = chunk(k, tall)
        both = []
        for which in range(2):
            here = slice(which * mid, (which + 1) * mid)
            x = [
                jnp.concatenate([lines[m, h, part, here] for h in range(2)], axis=1)
                for m in range(modes)
            ]
            both.append(after(jnp.concatenate(x, axis=0), inv, which))
        total, gap = both[0] + both[1], both[0] - both[1]
        sums = [jnp.zeros((tall, side), jnp.float32)] * 2
        for m in range(modes):
            here = slice(m * tall, (m + 1) * tall)
            new_real, new_imag = (
                jnp.concatenate(
                    [x[here, h * mid : (h + 1) * mid] for x in (total, gap)], axis=1
                )
                for h in range(2)
            )
            real, imag = (rolled[h, m, part] for h in range(2))
            sums[0] += real * new_real + imag * new_imag
            sums[1] += real * new_imag - imag * new_real
        for h in range(2):
            terms[h, part] = sums[h]

        @pl.when(has_right)
        def _():
            for j in range(k * per_tall, (k + 1) * per_tall):
                rights[j].start()

    thin_lane = lax.broadcasted_iota(jnp.int32, (OUT_ROWS, side), 1)
    thin_line = lax.broadcasted_iota(jnp.int32, (OUT_ROWS, side), 0)

    def share_out(j):
        part = chunk(j, OUT_ROWS)
        at = thin_line + j * OUT_ROWS
        for h in range(2):
            mine = jnp.where(thin_lane >= over, terms[h, part], 0.0)
            own[h, part] = jnp.where(at >= down, mine, 0.0)
            lower[h, part] = jnp.where(at < down, mine, 0.0)

        @pl.when(has_left)
        def _():
            rights[j].wait_recv()
            for h in range(2):
                other = jnp.where(thin_lane < left_over, left[h, part], 0.0)
                own[h, part] += jnp.where(at >= left_down, other, 0.0)
                lower[h, part] += jnp.where(at < left_down, other, 0.0)

        pl.when(has_below)(downs[j].start)

    def enter(j):
        @pl.when(jnp.logical_not(has_outer))
        def _():
            if layers == 2:
                swaps[j].start()
            else:
                inward[j].start()

    def gather(j):
        part = chunk(j, OUT_ROWS)

        @pl.when(has_outer)
        def _():
            inward[j].wait_recv()
            for h in range(2):
                own[h, part] += inbound[h, part]
            pl.when(is_hub)(swaps[j].start)
            pl.when(jnp.logical_not(is_hub))(inward[j].start)

    def finish(j):
        part = chunk(j, OUT_ROWS)

        @pl.when(is_hub)
        def _():
            swaps[j].wait_recv()
            for h in range(2):
                number = own[h, part] + crossed[h, part] + DAMPING * obj[h, part]
                out[h, part] = number * weight[part]
            pl.when(has_outer)(results[j].start)

    def chain(s):
        if s < steps:
            enter(s)
        if LAG_IN <= s < steps + LAG_IN:
            gather(s - LAG_IN)
        if s >= LAG_IN + LAG_CROSS:
            finish(s - LAG_IN - LAG_CROSS)

    def arrive(j):
        part = chunk(j, OUT_ROWS)

        @pl.when(has_above)
        def _():
            downs[j].wait_recv()
            for h in range(2):
                own[h, part] += upper[h, part]

    for k in range(PARTS):
        with scope(f"rb{k}"):
            rows_back(k)

    @pl.when(is_hub)
    def _():
        with scope("weight"):
            pl.when(has_above)(functools.partial(weigh, range(4)))
            weight[...] = 1.0 / weight[...]

    for s in range(steps + LAG_IN + LAG_CROSS):
        with scope(f"out{s}"):
            if s < steps:
                share_out(s)
                arrive(s)
            chain(s)

    @pl.when(jnp.logical_not(is_hub))
    def _():
        for j in range(steps):
            with scope(f"res{j}"):
                results[j].wait_recv()
                pl.when(has_outer)(results[j].start)

    def sent(there, src, send_sem):
        @pl.when(there)
        def _():
            send(src, src, s_send.at[send_sem], r_pass.at[0], east).wait_send()

    with scope("drain"):
        part = obj.at[:, :mid]
        sent(has_left, obj, 0)
        sent(has_above, part, 1)
        sent(has_below, part, 2)
        sent(has_below & has_left, part, 3)
        sent(has_below & has_left & odd_col, part, 4)
        sent(has_above & has_right & odd_col, part, 5)
        if layers > 1:
            sent(layers > 1, offs.at[0, pl.ds(0, layers - 1)], 6)
        sent(has_right, offs.at[0], 7)
        sent(has_below, offs.at[0], 8)
        sent(has_below & has_left, offs.at[0], 9)
        sent(has_right, terms, 10)
        sent(has_below, lower, 11)
        sent(jnp.logical_not(is_hub), own, 12)
        sent(is_hub, own, 13)
        sent(has_outer, out, 14)


def tables(side):
    mid = side // 2
    steps = np.arange(mid)
    kinds = []
    for shift in range(2):
        angle = (steps[:, None] * (2 * steps[None, :] + shift) % side) * (2.0 * np.pi / side)
        real, imag = np.cos(angle) / np.sqrt(side), -np.sin(angle) / np.sqrt(side)
        kinds.append(np.block([[real, imag], [-imag, real]]))
    both = np.stack(kinds)

    def halves(x):
        x = x.astype(np.float32)
        high = x.astype(jnp.bfloat16)
        return high, (x - high.astype(np.float32)).astype(jnp.bfloat16)

    return halves(both) + halves(both.transpose(0, 2, 1))


def body(sizes, object_field, probe_modes, amplitudes, offsets):
    rows, cols, layers = sizes
    side = object_field.shape[1]
    assert object_field.shape[2] == side and probe_modes.shape[2] == side
    assert offsets.shape[0] == 1 and layers % 2 == 0
    assert side % (PARTS * 2 * IN_ROWS) == 0 and side % (PARTS * OUT_ROWS) == 0
    modes = probe_modes.shape[1]
    hbm = pl.BlockSpec(memory_space=pltpu.MemorySpace.HBM)
    vmem = pl.BlockSpec(memory_space=pltpu.MemorySpace.VMEM)
    pair = (2, side, side)
    f32 = jnp.float32
    dma = pltpu.SemaphoreType.DMA
    tabs = tuple(jnp.asarray(t) for t in tables(side))
    tab = pltpu.VMEM((2, side, side), jnp.bfloat16)
    plane = pltpu.VMEM((side, side), f32)
    whole = pltpu.VMEM(pair, f32)
    corners = (4, layers, 1, 128)
    pieces, steps = side // IN_ROWS // 2, side // OUT_ROWS
    return pl.pallas_call(
        functools.partial(kernel, sizes),
        out_shape=pltpu.VMEM(pair, f32),
        in_specs=[hbm] * 8,
        out_specs=vmem,
        scratch_shapes=[
            pltpu.SMEM((1, 2), jnp.int32),
            whole,
            pltpu.VMEM(probe_modes.shape, f32),
            pltpu.VMEM((1, side, side), f32),
        ]
        + [tab] * 4
        + [pltpu.VMEM(corners, jnp.int32), pltpu.SMEM(corners, jnp.int32)]
        + [whole] * 3
        + [
            pltpu.VMEM(probe_modes.shape, f32),
            pltpu.VMEM((modes, 2, side, side), f32),
            pltpu.VMEM((modes, 2, side, side), f32),
        ]
        + [plane] * 3
        + [whole] * 7
        + [dma((8,)), dma(()), dma((15,)), dma((layers - 1,)), dma((3,))]
        + [dma((2 * pieces,))]
        + [dma((pieces,))] * 4
        + [dma((steps,))] * 4,
        compiler_params=pltpu.CompilerParams(
            collective_id=0, has_side_effects=True, vmem_limit_bytes=58 * 1024 * 1024
        ),
        name="update",
    )(offsets, object_field, probe_modes, amplitudes, *tabs)


def solution(mesh):
    sizes = tuple(mesh.shape[a] for a in AXES)
    placed = (
        P(None, "row", "col"),
        P(),
        P(("row", "col", "layer"), None, None),
        P(("row", "col", "layer"), None),
    )
    return jax.shard_map(
        functools.partial(body, sizes),
        mesh=mesh,
        in_specs=placed,
        out_specs=P(None, "row", "col"),
        check_vma=False,
    )
```

```python
import contextlib
import functools

import jax
import jax.numpy as jnp
import numpy as np
from jax import lax
from jax.experimental import pallas as pl
from jax.experimental.pallas import tpu as pltpu
from jax.sharding import PartitionSpec as P

SOFTEN = 0.05
DAMPING = 0.5
AXES = ("row", "col", "layer")
PARTS = 4
IN_ROWS = 16
UNROLL = 4
SIDE_ROWS = 16
OUT_ROWS = 16
LAG_IN = 8
LAG_CROSS = 7
GATE = 10


def scope(name):
    return contextlib.nullcontext()


def place():
    return tuple(lax.axis_index(a) for a in AXES)


def send(src, dst, send_sem, recv_sem, device):
    return pltpu.make_async_remote_copy(
        src_ref=src,
        dst_ref=dst,
        send_sem=send_sem,
        recv_sem=recv_sem,
        device_id=device,
        device_id_type=pl.DeviceIdType.MESH,
    )


def greet(rows, cols, layers):
    r, c, l = place()
    barrier = pltpu.get_barrier_semaphore()

    def tell(device):
        pl.semaphore_signal(
            barrier, inc=1, device_id=device, device_id_type=pl.DeviceIdType.MESH
        )

    near = (
        (c > 0, (r, c - 1, l)),
        (c < cols - 1, (r, c + 1, l)),
        (r > 0, (r - 1, c, l)),
        (r < rows - 1, (r + 1, c, l)),
        ((r > 0) & (c < cols - 1), (r - 1, c + 1, l)),
        ((r < rows - 1) & (c > 0), (r + 1, c - 1, l)),
    )
    for there, device in near:
        pl.when(there)(functools.partial(tell, device))
    for d in range(1, layers):
        tell((r, c, lax.rem(l + d, layers)))
    count = layers - 1
    for there, _ in near:
        count += there.astype(jnp.int32)
    pl.semaphore_wait(barrier, count)


def split(x):
    high = x.astype(jnp.bfloat16)
    return high, (x - high.astype(jnp.float32)).astype(jnp.bfloat16)


def prod(left, right):
    def one(a, b):
        return jnp.dot(a, b, preferred_element_type=jnp.float32)

    return one(left[0], right[0]) + (one(left[0], right[1]) + one(left[1], right[0]))


def corner_of(offs, group, layer, side):
    r, c, _ = place()
    tile_row = r - (1 if group >= 2 else 0)
    tile_col = c - (group % 2)
    return offs[group, layer, 0, 0] - tile_row * side, offs[group, layer, 0, 1] - tile_col * side


def kernel(
    sizes,
    corner_hbm, obj_hbm, probe_hbm, amp_hbm, fwd_high_hbm, fwd_low_hbm, inv_high_hbm, inv_low_hbm,
    out,
    corner, obj, probe, amp, fwd_high, fwd_low, inv_high, inv_low, offs, corners,
    right, below, diag, rolled, lines, far, ratio, power, weight,
    terms, left, own, lower, upper, inbound, crossed,
    s_load, s_corner, s_send, r_off, r_pass,
    r_right, r_right2, r_below, r_share, r_diag, r_diag2, r_left, r_down, r_in, r_last, gate,
):
    rows, cols, layers = sizes
    side = obj.shape[1]
    mid = side // 2
    modes = probe.shape[1]
    tall = side // PARTS
    pieces = side // IN_ROWS // 2
    steps = side // OUT_ROWS
    r, c, l = place()
    has_right, has_left = c < cols - 1, c > 0
    has_below, has_above = r < rows - 1, r > 0
    half = layers // 2
    low_half = l < half
    is_hub = (l == half - 1) | (l == half)
    has_outer = (l > 0) & (l < layers - 1)
    inner = (r, c, l + jnp.where(low_half, 1, -1))
    outer = (r, c, l + jnp.where(low_half, -1, 1))
    odd = lax.rem(l, 2)
    partner = (r, c, l + 1 - 2 * odd)
    west, east = (r, c - 1, l), (r, c + 1, l)
    north, south = (r - 1, c, l), (r + 1, c, l)
    odd_col = lax.rem(c, 2) == 1

    loads = [
        pltpu.make_async_copy(src, dst, s_load.at[i])
        for i, (src, dst) in enumerate(
            (
                (corner_hbm, corner),
                (obj_hbm, obj),
                (probe_hbm, probe),
                (amp_hbm, amp),
                (fwd_high_hbm, fwd_high),
                (fwd_low_hbm, fwd_low),
                (inv_high_hbm, inv_high),
                (inv_low_hbm, inv_low),
            )
        )
    ]
    for copy in loads:
        copy.start()
    with scope("greet"):
        greet(rows, cols, layers)
    with scope("load"):
        loads[1].wait()

    def chunk(k, size):
        return pl.ds(k * size, size)

    def piece(src, dst, part, send_sem, recv_sem, device):
        return send(src.at[:, part], dst.at[:, part], s_send.at[send_sem], recv_sem, device)

    lefts, lefts2, ups, shares, diags, diags2, extras = [], [], [], [], [], [], []
    for i in range(pieces):
        mine, other = chunk(2 * i + odd, IN_ROWS), chunk(2 * i + 1 - odd, IN_ROWS)
        lefts.append(piece(obj, right, mine, 0, r_right.at[i // 2], west))
        lefts2.append(piece(obj, right, other, 0, r_right2.at[i // 2], west))
        ups.append(piece(obj, below, mine, 1, r_below.at[i], north))
        shares.append(piece(below, below, mine, 2, r_share.at[i], partner))
        diags.append(piece(below, diag, mine, 3, r_diag.at[i // 2], west))
        diags2.append(piece(below, diag, other, 4, r_diag2.at[i // 2], west))
        extras.append(piece(right, diag, other, 5, r_diag2.at[i // 2], north))

    def two(recv_sem):
        piece(obj, right, chunk(0, 2 * IN_ROWS), 0, recv_sem, west).wait_recv()

    for copy in ups:
        pl.when(has_above)(copy.start)
    for copy in lefts2 + lefts:
        pl.when(has_left)(copy.start)
    with scope("load0"):
        loads[0].wait()
    at = lax.broadcasted_iota(jnp.int32, (1, 1, 128), 2)
    offs[0, pl.ds(l, 1)] = jnp.where(at == 0, corner[0, 0], corner[0, 1])
    mine = offs.at[0, pl.ds(l, 1)]
    around = [(d, lax.rem(l + d, layers)) for d in range(1, layers)]
    peers = [send(mine, mine, s_send.at[6], r_off.at[d - 1], (r, c, p)) for d, p in around]
    for peer in peers:
        peer.start()
    down = corner[0, 0] - r * side
    over = corner[0, 1] - c * side
    with scope("load2"):
        loads[2].wait()

    def prepare(m):
        for h in range(2):
            rolled[h, m] = pltpu.roll(pltpu.roll(probe[h, m], down, 0), over, 1)

    def forward(i):
        @pl.when(has_below)
        def _():
            ups[i].wait_recv()
            shares[i].start()
            pl.when(has_left)(diags[i].start)

        if i % 2 == 0:

            @pl.when(has_above & has_right & odd_col)
            def _():
                two(r_right2.at[i // 2])
                extras[i].start()
                extras[i + 1].start()

    def forward2(i):
        @pl.when(has_below)
        def _():
            shares[i].wait_recv()
            pl.when(has_left & odd_col)(diags2[i].start)

    across = send(offs.at[0], offs.at[1], s_send.at[7], r_pass.at[0], east)
    down0 = send(offs.at[0], offs.at[2], s_send.at[8], r_pass.at[1], south)
    down1 = send(offs.at[1], offs.at[3], s_send.at[9], r_pass.at[2], south)

    def weigh(groups, first=0, last=layers):
        there = (None, has_left, has_above, has_left & has_above)
        wide = lax.broadcasted_iota(jnp.int32, (side, side), 1)
        deep = lax.broadcasted_iota(jnp.int32, (side, side), 0)
        for group in groups:

            def add(layer, carry, group=group):
                a, b = corner_of(corners, group, layer, side)
                window = pltpu.roll(pltpu.roll(power[...], a, 0), b, 1)
                keep = (deep < a) if group >= 2 else (deep >= a)
                keep &= (wide < b) if group % 2 else (wide >= b)
                weight[...] += jnp.where(keep, window, 0.0)
                return carry

            def all_layers(add=add):
                lax.fori_loop(first, last, add, 0)

            if there[group] is None:
                all_layers()
            else:
                pl.when(there[group])(all_layers)

    def fetch():
        copy = pltpu.make_async_copy(offs, corners, s_corner)
        copy.start()
        copy.wait()

    fetched = pltpu.make_async_copy(offs, corners, s_corner)

    with scope("prep"):
        for m in range(modes):
            prepare(m)
    with scope("amp"):
        power[...] = jnp.zeros_like(power)
        for m in range(modes):
            power[...] += probe[0, m] * probe[0, m] + probe[1, m] * probe[1, m]
        loads[3].wait()
        wide = lax.broadcasted_iota(jnp.int32, (side, side), 1)
        deep = lax.broadcasted_iota(jnp.int32, (side, side), 0)

        def pick(to, start):
            return to == jnp.where(start < mid, 2 * start, 2 * start - side + 1)

        turn = jnp.where(pick(wide, deep), 1.0, 0.0).astype(jnp.bfloat16)
        back_turn = jnp.where(pick(deep, wide), 1.0, 0.0).astype(jnp.bfloat16)

        def moved(x, along):
            total = None
            for _ in range(3):
                high = x.astype(jnp.bfloat16)
                x = x - high.astype(jnp.float32)
                pair = (turn, high) if along == 0 else (high, back_turn)
                one = jnp.dot(*pair, preferred_element_type=jnp.float32)
                total = one if total is None else total + one
            return total

        amp[0] = moved(moved(amp[0], 0), 1)
        weight[...] = jnp.full_like(weight, DAMPING)

    with scope("peers"):
        for peer in peers:
            peer.wait_recv()
        pl.when(has_right)(across.start)
    with scope("fwd0"):
        forward(0)
    for i in (1, 2):
        with scope(f"fwd{i}"):
            forward(i)
    with scope("across"):

        @pl.when(has_left)
        def _():
            across.wait_recv()

        @pl.when(jnp.logical_not(has_left))
        def _():
            offs[1] = jnp.zeros(offs.shape[1:], jnp.int32)

        @pl.when(has_below)
        def _():
            down0.start()
            pl.when(has_left)(down1.start)

        @pl.when(jnp.logical_not(has_above))
        def _():
            offs[2] = jnp.zeros(offs.shape[1:], jnp.int32)
            offs[3] = jnp.zeros(offs.shape[1:], jnp.int32)
            fetched.start()

    fwd, inv = (fwd_high, fwd_low), (inv_high, inv_low)

    def after(x, table, which):
        return prod(split(x), (table[0][which], table[1][which]))

    def ahead(table, which, x):
        return prod((table[0][which], table[1][which]), split(x))

    lane = lax.broadcasted_iota(jnp.int32, (tall, side), 1)
    line = lax.broadcasted_iota(jnp.int32, (tall, side), 0)

    def first_part(k):
        part = chunk(k, tall)
        with scope(f"merge{k}"):
            high = line + k * tall < down
            for h in range(2):
                own[h, part] = obj[h, part]

            @pl.when(has_right & jnp.logical_not(has_above & odd_col))
            def _():
                two(r_right2.at[k])

            @pl.when(has_right)
            def _():
                two(r_right.at[k])
                for h in range(2):
                    own[h, part] = jnp.where(lane < over, right[h, part], own[h, part])

            @pl.when(has_below)
            def _():
                for h in range(2):
                    own[h, part] = jnp.where(high & (lane >= over), below[h, part], own[h, part])

            @pl.when(has_below & has_right)
            def _():
                two(r_diag.at[k])
                two(r_diag2.at[k])
                for h in range(2):
                    own[h, part] = jnp.where(high & (lane < over), diag[h, part], own[h, part])

        with scope(f"first{k}"):
            patch = [own[h, part] for h in range(2)]
            sums, gaps = [], []
            for m in range(modes):
                real, imag = (rolled[h, m, part] for h in range(2))
                new = (real * patch[0] - imag * patch[1], real * patch[1] + imag * patch[0])
                sums.append(jnp.concatenate([x[:, :mid] + x[:, mid:] for x in new], axis=1))
                gaps.append(jnp.concatenate([x[:, :mid] - x[:, mid:] for x in new], axis=1))
            even = after(jnp.concatenate(sums, axis=0), fwd, 0)
            uneven = after(jnp.concatenate(gaps, axis=0), fwd, 1)
            for m in range(modes):
                here = slice(m * tall, (m + 1) * tall)
                for h in range(2):
                    there = slice(h * mid, (h + 1) * mid)
                    lines[m, h, part] = jnp.concatenate(
                        [even[here, there], uneven[here, there]], axis=1
                    )

    early = has_below & jnp.logical_not(odd_col & has_right)
    quarters = [(g, q * layers // 2, (q + 1) * layers // 2) for g in (0, 1) for q in range(2)]
    with scope("loads"):
        for copy in loads[4:]:
            copy.wait()
    for i in range(3, pieces):
        with scope(f"fwd{i}"):
            forward(i)
    for i in range(pieces):
        with scope(f"fwz{i}"):
            forward2(i)
        if i < 4:

            @pl.when(jnp.logical_not(has_above) & is_hub)
            def _(i=i):
                with scope(f"weight{i}"):
                    if i == 0:
                        fetched.wait()
                    group, start, stop = quarters[i]
                    weigh((group,), start, stop)

        if i % 2 == 1 and i > 1:
            pl.when(early)(functools.partial(first_part, i // 2 - 1))
    pl.when(early)(functools.partial(first_part, PARTS - 1))
    pl.when(jnp.logical_not(has_above | is_hub))(fetched.wait)

    @pl.when(jnp.logical_not(early))
    def _():
        for k in range(PARTS):
            first_part(k)

    ratio[...] = jnp.zeros_like(ratio)

    def columns(m, carry):
        x = [lines[m, h] for h in range(2)]
        sums = jnp.concatenate([p[:mid] + p[mid:] for p in x], axis=0)
        gaps = jnp.concatenate([p[:mid] - p[mid:] for p in x], axis=0)
        for which, y in enumerate((sums, gaps)):
            spread = ahead(inv, which, y)
            far[m, which] = spread
            here = slice(which * mid, (which + 1) * mid)
            ratio[here] += spread[:mid] * spread[:mid] + spread[mid:] * spread[mid:]
        return carry

    with scope("columns"):
        lax.fori_loop(0, modes, columns, 0, unroll=UNROLL)
    ratio[...] = amp[0] / (jnp.sqrt(ratio[...]) + SOFTEN)

    def back(m, carry):
        turned = []
        for which in range(2):
            scale = ratio[which * mid : (which + 1) * mid]
            fixed = jnp.concatenate([far[m, which, :mid] * scale, far[m, which, mid:] * scale], axis=0)
            turned.append(ahead(fwd, which, fixed))
        total, gap = turned[0] + turned[1], turned[0] - turned[1]
        for h in range(2):
            there = slice(h * mid, (h + 1) * mid)
            lines[m, h, :mid] = total[there]
            lines[m, h, mid:] = gap[there]
        return carry

    with scope("back"):
        lax.fori_loop(0, modes, back, 0, unroll=UNROLL)

    @pl.when(has_above)
    def _():
        with scope("fetch"):
            down0.wait_recv()
            pl.when(has_left)(down1.wait_recv)

            @pl.when(jnp.logical_not(has_left))
            def _():
                offs[3] = jnp.zeros(offs.shape[1:], jnp.int32)

            fetched.start()
            fetched.wait()

    left_down, left_over = corner_of(corners, 1, l, side)

    def flow(src, dst, send_sem, recv_sem, device, size=OUT_ROWS):
        return [
            piece(src, dst, chunk(k, size), send_sem, recv_sem.at[k], device)
            for k in range(side // size)
        ]

    rights = flow(terms, left, 10, r_left, east, SIDE_ROWS)
    downs = flow(lower, upper, 11, r_down, south)
    inward = flow(own, inbound, 12, r_in, inner)
    swaps = flow(own, crossed, 13, r_last, inner)
    results = flow(out, out, 14, r_last, outer)
    per_tall = tall // SIDE_ROWS
    per_side = SIDE_ROWS // OUT_ROWS

    def rows_back(k):
        part = chunk(k, tall)
        both = []
        for which in range(2):
            here = slice(which * mid, (which + 1) * mid)
            x = [
                jnp.concatenate([lines[m, h, part, here] for h in range(2)], axis=1)
                for m in range(modes)
            ]
            both.append(after(jnp.concatenate(x, axis=0), inv, which))
        total, gap = both[0] + both[1], both[0] - both[1]
        sums = [jnp.zeros((tall, side), jnp.float32)] * 2
        for m in range(modes):
            here = slice(m * tall, (m + 1) * tall)
            new_real, new_imag = (
                jnp.concatenate(
                    [x[here, h * mid : (h + 1) * mid] for x in (total, gap)], axis=1
                )
                for h in range(2)
            )
            real, imag = (rolled[h, m, part] for h in range(2))
            sums[0] += real * new_real + imag * new_imag
            sums[1] += real * new_imag - imag * new_real
        for h in range(2):
            terms[h, part] = sums[h]

        @pl.when(has_right)
        def _():
            for j in range(k * per_tall, (k + 1) * per_tall):
                rights[j].start()

    thin_lane = lax.broadcasted_iota(jnp.int32, (OUT_ROWS, side), 1)
    thin_line = lax.broadcasted_iota(jnp.int32, (OUT_ROWS, side), 0)

    def share_out(j):
        part = chunk(j, OUT_ROWS)
        at = thin_line + j * OUT_ROWS
        for h in range(2):
            mine = jnp.where(thin_lane >= over, terms[h, part], 0.0)
            own[h, part] = jnp.where(at >= down, mine, 0.0)
            lower[h, part] = jnp.where(at < down, mine, 0.0)

        @pl.when(has_left)
        def _():
            if j % per_side == 0:
                rights[j // per_side].wait_recv()
            for h in range(2):
                other = jnp.where(thin_lane < left_over, left[h, part], 0.0)
                own[h, part] += jnp.where(at >= left_down, other, 0.0)
                lower[h, part] += jnp.where(at < left_down, other, 0.0)

        pl.when(has_below)(downs[j].start)

    def enter(j):
        @pl.when(jnp.logical_not(has_outer))
        def _():
            if layers == 2:
                swaps[j].start()
            else:
                inward[j].start()

    def gather(j):
        part = chunk(j, OUT_ROWS)

        @pl.when(has_outer)
        def _():
            inward[j].wait_recv()
            for h in range(2):
                own[h, part] += inbound[h, part]
            pl.when(is_hub)(swaps[j].start)
            pl.when(jnp.logical_not(is_hub))(inward[j].start)

    def finish(j):
        part = chunk(j, OUT_ROWS)

        @pl.when(is_hub)
        def _():
            swaps[j].wait_recv()
            for h in range(2):
                number = own[h, part] + crossed[h, part] + DAMPING * obj[h, part]
                out[h, part] = number * weight[part]
            pl.when(has_outer)(results[j].start)

    def chain(s):
        if s < steps:
            enter(s)
        if LAG_IN <= s < steps + LAG_IN:
            gather(s - LAG_IN)
        if s >= LAG_IN + LAG_CROSS:
            finish(s - LAG_IN - LAG_CROSS)

    def arrive(j):
        part = chunk(j, OUT_ROWS)

        @pl.when(has_above)
        def _():
            downs[j].wait_recv()
            for h in range(2):
                own[h, part] += upper[h, part]
            if j == GATE:

                @pl.when(jnp.logical_not(odd_col) & has_right)
                def _():
                    pl.semaphore_signal(
                        gate, 1, device_id=(r - 1, c + 1, l), device_id_type=pl.DeviceIdType.MESH
                    )

    for k in range(PARTS):
        with scope(f"rb{k}"):
            rows_back(k)

    @pl.when(is_hub)
    def _():
        with scope("weight"):
            pl.when(has_above)(functools.partial(weigh, range(4)))
            weight[...] = 1.0 / weight[...]

    @pl.when(has_below & odd_col)
    def _():
        with scope("gate"):
            pl.semaphore_wait(gate, 1)

    for s in range(steps + LAG_IN + LAG_CROSS):
        with scope(f"out{s}"):
            if s < steps:
                share_out(s)
                arrive(s)
            chain(s)

    @pl.when(jnp.logical_not(is_hub))
    def _():
        for j in range(steps):
            with scope(f"res{j}"):
                results[j].wait_recv()
                pl.when(has_outer)(results[j].start)

    def sent(there, src, send_sem):
        @pl.when(there)
        def _():
            send(src, src, s_send.at[send_sem], r_pass.at[0], east).wait_send()

    with scope("drain"):
        part = obj.at[:, :mid]
        sent(has_left, obj, 0)
        sent(has_above, part, 1)
        sent(has_below, part, 2)
        sent(has_below & has_left, part, 3)
        sent(has_below & has_left & odd_col, part, 4)
        sent(has_above & has_right & odd_col, part, 5)
        if layers > 1:
            sent(layers > 1, offs.at[0, pl.ds(0, layers - 1)], 6)
        sent(has_right, offs.at[0], 7)
        sent(has_below, offs.at[0], 8)
        sent(has_below & has_left, offs.at[0], 9)
        sent(has_right, terms, 10)
        sent(has_below, lower, 11)
        sent(jnp.logical_not(is_hub), own, 12)
        sent(is_hub, own, 13)
        sent(has_outer, out, 14)


def tables(side):
    mid = side // 2
    steps = np.arange(mid)
    kinds = []
    for shift in range(2):
        angle = (steps[:, None] * (2 * steps[None, :] + shift) % side) * (2.0 * np.pi / side)
        real, imag = np.cos(angle) / np.sqrt(side), -np.sin(angle) / np.sqrt(side)
        kinds.append(np.block([[real, imag], [-imag, real]]))
    both = np.stack(kinds)

    def halves(x):
        x = x.astype(np.float32)
        high = x.astype(jnp.bfloat16)
        return high, (x - high.astype(np.float32)).astype(jnp.bfloat16)

    return halves(both) + halves(both.transpose(0, 2, 1))


def body(sizes, object_field, probe_modes, amplitudes, offsets):
    rows, cols, layers = sizes
    side = object_field.shape[1]
    assert object_field.shape[2] == side and probe_modes.shape[2] == side
    assert offsets.shape[0] == 1 and layers % 2 == 0
    assert side == PARTS * 4 * IN_ROWS
    assert side % (PARTS * SIDE_ROWS) == 0 and SIDE_ROWS % OUT_ROWS == 0
    modes = probe_modes.shape[1]
    hbm = pl.BlockSpec(memory_space=pltpu.MemorySpace.HBM)
    vmem = pl.BlockSpec(memory_space=pltpu.MemorySpace.VMEM)
    pair = (2, side, side)
    f32 = jnp.float32
    dma = pltpu.SemaphoreType.DMA
    tabs = tuple(jnp.asarray(t) for t in tables(side))
    tab = pltpu.VMEM((2, side, side), jnp.bfloat16)
    plane = pltpu.VMEM((side, side), f32)
    whole = pltpu.VMEM(pair, f32)
    corners = (4, layers, 1, 128)
    pieces, steps = side // IN_ROWS // 2, side // OUT_ROWS
    return pl.pallas_call(
        functools.partial(kernel, sizes),
        out_shape=pltpu.VMEM(pair, f32),
        in_specs=[hbm] * 8,
        out_specs=vmem,
        scratch_shapes=[
            pltpu.SMEM((1, 2), jnp.int32),
            whole,
            pltpu.VMEM(probe_modes.shape, f32),
            pltpu.VMEM((1, side, side), f32),
        ]
        + [tab] * 4
        + [pltpu.VMEM(corners, jnp.int32), pltpu.SMEM(corners, jnp.int32)]
        + [whole] * 3
        + [
            pltpu.VMEM(probe_modes.shape, f32),
            pltpu.VMEM((modes, 2, side, side), f32),
            pltpu.VMEM((modes, 2, side, side), f32),
        ]
        + [plane] * 3
        + [whole] * 7
        + [dma((8,)), dma(()), dma((15,)), dma((layers - 1,)), dma((3,))]
        + [dma((pieces // 2,))] * 2
        + [dma((pieces,))] * 2
        + [dma((pieces // 2,))] * 2
        + [dma((side // SIDE_ROWS,))]
        + [dma((steps,))] * 3
        + [pltpu.SemaphoreType.REGULAR],
        compiler_params=pltpu.CompilerParams(
            collective_id=0, has_side_effects=True, vmem_limit_bytes=58 * 1024 * 1024
        ),
        name="update",
    )(offsets, object_field, probe_modes, amplitudes, *tabs)


def solution(mesh):
    sizes = tuple(mesh.shape[a] for a in AXES)
    placed = (
        P(None, "row", "col"),
        P(),
        P(("row", "col", "layer"), None, None),
        P(("row", "col", "layer"), None),
    )
    return jax.shard_map(
        functools.partial(body, sizes),
        mesh=mesh,
        in_specs=placed,
        out_specs=P(None, "row", "col"),
        check_vma=False,
    )
```

```python
import contextlib
import functools

import jax
import jax.numpy as jnp
import numpy as np
from jax import lax
from jax.experimental import pallas as pl
from jax.experimental.pallas import tpu as pltpu
from jax.sharding import PartitionSpec as P

SOFTEN = 0.05
DAMPING = 0.5
AXES = ("row", "col", "layer")
PARTS = 4
IN_ROWS = 16
UNROLL = 4
OUT_ROWS = 16
LAG_IN = 8
LAG_CROSS = 7
GATE = 7
HEAD = 4
OVER_SIDE = 6


def scope(name):
    return contextlib.nullcontext()


def place():
    return tuple(lax.axis_index(a) for a in AXES)


def send(src, dst, send_sem, recv_sem, device):
    return pltpu.make_async_remote_copy(
        src_ref=src,
        dst_ref=dst,
        send_sem=send_sem,
        recv_sem=recv_sem,
        device_id=device,
        device_id_type=pl.DeviceIdType.MESH,
    )


def greet(rows, cols, layers):
    r, c, l = place()
    barrier = pltpu.get_barrier_semaphore()

    def tell(device):
        pl.semaphore_signal(
            barrier, inc=1, device_id=device, device_id_type=pl.DeviceIdType.MESH
        )

    near = (
        (c > 0, (r, c - 1, l)),
        (c < cols - 1, (r, c + 1, l)),
        (r > 0, (r - 1, c, l)),
        (r < rows - 1, (r + 1, c, l)),
        ((r > 0) & (c < cols - 1), (r - 1, c + 1, l)),
        ((r < rows - 1) & (c > 0), (r + 1, c - 1, l)),
    )
    for there, device in near:
        pl.when(there)(functools.partial(tell, device))
    for d in range(1, layers):
        tell((r, c, lax.rem(l + d, layers)))
    count = layers - 1
    for there, _ in near:
        count += there.astype(jnp.int32)
    pl.semaphore_wait(barrier, count)


def split(x):
    high = x.astype(jnp.bfloat16)
    return high, (x - high.astype(jnp.float32)).astype(jnp.bfloat16)


def prod(left, right):
    def one(a, b):
        return jnp.dot(a, b, preferred_element_type=jnp.float32)

    return one(left[0], right[0]) + (one(left[0], right[1]) + one(left[1], right[0]))


def corner_of(offs, group, layer, side):
    r, c, _ = place()
    tile_row = r - (1 if group >= 2 else 0)
    tile_col = c - (group % 2)
    return offs[group, layer, 0, 0] - tile_row * side, offs[group, layer, 0, 1] - tile_col * side


def kernel(
    sizes,
    corner_hbm, obj_hbm, probe_hbm, amp_hbm, table_hbm,
    out,
    corner, obj, probe, amp, table, offs, corners,
    right, below, diag, rolled, lines, far, parted, ratio, power, weight,
    terms, left, own, lower, upper, inbound, crossed,
    s_load, s_corner, s_send, r_off, r_pass,
    r_right, r_right2, r_pool, r_left, r_in, r_last, gate,
):
    rows, cols, layers = sizes
    side = obj.shape[1]
    mid = side // 2
    modes = probe.shape[1]
    tall = side // PARTS
    pieces = side // IN_ROWS // 2
    steps = side // OUT_ROWS
    r, c, l = place()
    has_right, has_left = c < cols - 1, c > 0
    has_below, has_above = r < rows - 1, r > 0
    half = layers // 2
    low_half = l < half
    is_hub = (l == half - 1) | (l == half)
    has_outer = (l > 0) & (l < layers - 1)
    inner = (r, c, l + jnp.where(low_half, 1, -1))
    outer = (r, c, l + jnp.where(low_half, -1, 1))
    odd = lax.rem(l, 2)
    partner = (r, c, l + 1 - 2 * odd)
    west, east = (r, c - 1, l), (r, c + 1, l)
    north, south = (r - 1, c, l), (r + 1, c, l)
    odd_col = lax.rem(c, 2) == 1

    loads = [
        pltpu.make_async_copy(src, dst, s_load.at[i])
        for i, (src, dst) in enumerate(
            (
                (corner_hbm, corner),
                (obj_hbm, obj),
                (probe_hbm, probe),
                (amp_hbm, amp),
                (table_hbm, table),
            )
        )
    ]
    for copy in loads:
        copy.start()
    with scope("greet"):
        greet(rows, cols, layers)
    with scope("load"):
        loads[1].wait()

    def chunk(k, size):
        return pl.ds(k * size, size)

    def piece(src, dst, part, send_sem, recv_sem, device):
        return send(src.at[:, part], dst.at[:, part], s_send.at[send_sem], recv_sem, device)

    lefts, lefts2, ups, shares, diags, diags2, extras, extras2 = ([] for _ in range(8))
    for i in range(pieces):
        mine, other = chunk(2 * i + odd, IN_ROWS), chunk(2 * i + 1 - odd, IN_ROWS)
        lefts.append(piece(obj, right, mine, 0, r_right.at[i // 2], west))
        lefts2.append(piece(obj, right, other, 0, r_right2.at[i // 2], west))
        ups.append(piece(obj, below, mine, 1, r_pool.at[i], north))
        shares.append(piece(below, below, mine, 2, r_pool.at[pieces + i], partner))
        diags.append(piece(below, diag, mine, 3, r_pool.at[2 * pieces + i // 2], west))
        diags2.append(piece(below, diag, other, 4, r_pool.at[2 * pieces + (pieces + i) // 2], west))
        if i >= OVER_SIDE:
            extras2.append(piece(right, diag, mine, 5, r_pool.at[2 * pieces + i // 2], north))
        extras.append(piece(right, diag, other, 5, r_pool.at[2 * pieces + (pieces + i) // 2], north))

    def two(recv_sem):
        piece(obj, right, chunk(0, 2 * IN_ROWS), 0, recv_sem, west).wait_recv()

    for copy in ups:
        pl.when(has_above)(copy.start)
    for copy in lefts2 + lefts[OVER_SIDE:] + lefts[:OVER_SIDE]:
        pl.when(has_left)(copy.start)
    with scope("load0"):
        loads[0].wait()
    at = lax.broadcasted_iota(jnp.int32, (1, 1, 128), 2)
    offs[0, pl.ds(l, 1)] = jnp.where(at == 0, corner[0, 0], corner[0, 1])
    mine = offs.at[0, pl.ds(l, 1)]
    around = [(d, lax.rem(l + d, layers)) for d in range(1, layers)]
    peers = [send(mine, mine, s_send.at[6], r_off.at[d - 1], (r, c, p)) for d, p in around]
    for peer in peers:
        peer.start()
    down = corner[0, 0] - r * side
    over = corner[0, 1] - c * side
    with scope("load2"):
        loads[2].wait()

    def prepare(m):
        for h in range(2):
            rolled[h, m] = pltpu.roll(pltpu.roll(probe[h, m], down, 0), over, 1)

    def forward(i):
        @pl.when(has_below)
        def _():
            ups[i].wait_recv()
            shares[i].start()
            pl.when(has_left & odd_col if i >= OVER_SIDE else has_left)(diags[i].start)

        if i % 2 == 0:

            @pl.when(has_above & has_right & odd_col)
            def _():
                two(r_right2.at[i // 2])
                extras[i].start()
                extras[i + 1].start()
                if i + 2 == pieces:
                    for k in range(OVER_SIDE // 2, pieces // 2):
                        two(r_right.at[k])
                    for copy in extras2:
                        copy.start()

    def forward2(i):
        @pl.when(has_below)
        def _():
            shares[i].wait_recv()
            pl.when(has_left & odd_col)(diags2[i].start)

    across = send(offs.at[0], offs.at[1], s_send.at[7], r_pass.at[0], east)
    down0 = send(offs.at[0], offs.at[2], s_send.at[8], r_pass.at[1], south)
    down1 = send(offs.at[1], offs.at[3], s_send.at[9], r_pass.at[2], south)

    def weigh(groups, first=0, last=layers):
        there = (None, has_left, has_above, has_left & has_above)
        wide = lax.broadcasted_iota(jnp.int32, (side, side), 1)
        deep = lax.broadcasted_iota(jnp.int32, (side, side), 0)
        for group in groups:

            def add(layer, carry, group=group):
                a, b = corner_of(corners, group, layer, side)
                window = pltpu.roll(pltpu.roll(power[...], a, 0), b, 1)
                keep = (deep < a) if group >= 2 else (deep >= a)
                keep &= (wide < b) if group % 2 else (wide >= b)
                weight[...] += jnp.where(keep, window, 0.0)
                return carry

            def all_layers(add=add):
                lax.fori_loop(first, last, add, 0)

            if there[group] is None:
                all_layers()
            else:
                pl.when(there[group])(all_layers)

    def fetch():
        copy = pltpu.make_async_copy(offs, corners, s_corner)
        copy.start()
        copy.wait()

    fetched = pltpu.make_async_copy(offs, corners, s_corner)

    with scope("prep"):
        for m in range(modes):
            prepare(m)
    with scope("amp"):
        power[...] = jnp.zeros_like(power)
        for m in range(modes):
            power[...] += probe[0, m] * probe[0, m] + probe[1, m] * probe[1, m]
        loads[3].wait()
        wide = lax.broadcasted_iota(jnp.int32, (side, side), 1)
        deep = lax.broadcasted_iota(jnp.int32, (side, side), 0)

        def pick(to, start):
            return to == jnp.where(start < mid, 2 * start, 2 * start - side + 1)

        turn = jnp.where(pick(wide, deep), 1.0, 0.0).astype(jnp.bfloat16)
        back_turn = jnp.where(pick(deep, wide), 1.0, 0.0).astype(jnp.bfloat16)

        def moved(x, along):
            total = None
            for _ in range(3):
                high = x.astype(jnp.bfloat16)
                x = x - high.astype(jnp.float32)
                pair = (turn, high) if along == 0 else (high, back_turn)
                one = jnp.dot(*pair, preferred_element_type=jnp.float32)
                total = one if total is None else total + one
            return total

        amp[0] = moved(moved(amp[0], 0), 1)
        weight[...] = jnp.full_like(weight, DAMPING)

    with scope("peers"):
        for peer in peers:
            peer.wait_recv()
        pl.when(has_right)(across.start)
    with scope("fwd0"):
        forward(0)
    for i in (1, 2):
        with scope(f"fwd{i}"):
            forward(i)
    with scope("across"):

        @pl.when(has_left)
        def _():
            across.wait_recv()

        @pl.when(jnp.logical_not(has_left))
        def _():
            offs[1] = jnp.zeros(offs.shape[1:], jnp.int32)

        @pl.when(has_below)
        def _():
            down0.start()
            pl.when(has_left)(down1.start)

        @pl.when(jnp.logical_not(has_above))
        def _():
            offs[2] = jnp.zeros(offs.shape[1:], jnp.int32)
            offs[3] = jnp.zeros(offs.shape[1:], jnp.int32)
            fetched.start()

    fwd, inv = (table.at[0], table.at[1]), (table.at[2], table.at[3])

    def after(x, table, which):
        return prod(split(x), (table[0][which], table[1][which]))

    def ahead(table, which, x):
        return prod((table[0][which], table[1][which]), split(x))

    lane = lax.broadcasted_iota(jnp.int32, (tall, side), 1)
    line = lax.broadcasted_iota(jnp.int32, (tall, side), 0)

    def first_part(k):
        part = chunk(k, tall)
        with scope(f"merge{k}"):
            high = line + k * tall < down
            for h in range(2):
                own[h, part] = obj[h, part]

            @pl.when(has_right & jnp.logical_not(has_above & odd_col))
            def _():
                two(r_right2.at[k])

            ready = has_above & odd_col if k >= OVER_SIDE // 2 else has_right & False
            pl.when(has_right & jnp.logical_not(ready))(lambda: two(r_right.at[k]))

            @pl.when(has_right)
            def _():
                for h in range(2):
                    own[h, part] = jnp.where(lane < over, right[h, part], own[h, part])

            @pl.when(has_below)
            def _():
                for h in range(2):
                    own[h, part] = jnp.where(high & (lane >= over), below[h, part], own[h, part])

            @pl.when(has_below & has_right)
            def _():
                two(r_pool.at[2 * pieces + k])
                two(r_pool.at[2 * pieces + pieces // 2 + k])
                for h in range(2):
                    own[h, part] = jnp.where(high & (lane < over), diag[h, part], own[h, part])

        with scope(f"first{k}"):
            patch = [own[h, part] for h in range(2)]
            sums, gaps = [], []
            for m in range(modes):
                real, imag = (rolled[h, m, part] for h in range(2))
                new = (real * patch[0] - imag * patch[1], real * patch[1] + imag * patch[0])
                sums.append(jnp.concatenate([x[:, :mid] + x[:, mid:] for x in new], axis=1))
                gaps.append(jnp.concatenate([x[:, :mid] - x[:, mid:] for x in new], axis=1))
            even = after(jnp.concatenate(sums, axis=0), fwd, 0)
            uneven = after(jnp.concatenate(gaps, axis=0), fwd, 1)
            for m in range(modes):
                here = slice(m * tall, (m + 1) * tall)
                for h in range(2):
                    there = slice(h * mid, (h + 1) * mid)
                    lines[m, h, part] = jnp.concatenate(
                        [even[here, there], uneven[here, there]], axis=1
                    )

    early = has_below & jnp.logical_not(odd_col & has_right)
    quarters = [(g, q * layers // 2, (q + 1) * layers // 2) for g in (0, 1) for q in range(2)]
    with scope("loads"):
        for copy in loads[4:]:
            copy.wait()
    for i in range(3, pieces):
        with scope(f"fwd{i}"):
            forward(i)
    for i in range(pieces):
        with scope(f"fwz{i}"):
            forward2(i)
        if i < 4:

            @pl.when(jnp.logical_not(has_above) & is_hub)
            def _(i=i):
                with scope(f"weight{i}"):
                    if i == 0:
                        fetched.wait()
                    group, start, stop = quarters[i]
                    weigh((group,), start, stop)

        if i % 2 == 1 and i > 1:
            pl.when(early)(functools.partial(first_part, i // 2 - 1))
    pl.when(early)(functools.partial(first_part, PARTS - 1))
    pl.when(jnp.logical_not(has_above | is_hub))(fetched.wait)

    @pl.when(jnp.logical_not(early))
    def _():
        for k in range(PARTS):
            first_part(k)

    ratio[...] = jnp.zeros_like(ratio)

    def columns(m, carry):
        x = [lines[m, h] for h in range(2)]
        sums = jnp.concatenate([p[:mid] + p[mid:] for p in x], axis=0)
        gaps = jnp.concatenate([p[:mid] - p[mid:] for p in x], axis=0)
        for which, y in enumerate((sums, gaps)):
            spread = ahead(inv, which, y)
            far[m, which] = spread
            here = slice(which * mid, (which + 1) * mid)
            ratio[here] += spread[:mid] * spread[:mid] + spread[mid:] * spread[mid:]
        return carry

    with scope("columns"):
        lax.fori_loop(0, modes, columns, 0, unroll=UNROLL)
    ratio[...] = amp[0] / (jnp.sqrt(ratio[...]) + SOFTEN)

    def back(p):
        near = (slice(p * tall, (p + 1) * tall), slice(mid + p * tall, mid + (p + 1) * tall))
        for m in range(modes):
            turned = []
            for which in range(2):
                if p == 0:
                    scale = ratio[which * mid : (which + 1) * mid]
                    fixed = jnp.concatenate(
                        [far[m, which, :mid] * scale, far[m, which, mid:] * scale], axis=0
                    )
                    halves = split(fixed)
                    for x in range(2):
                        parted[x, m, which] = halves[x]
                else:
                    halves = (parted[0, m, which], parted[1, m, which])
                rows_of = [
                    jnp.concatenate([t[which, here] for here in near], axis=0) for t in fwd
                ]
                turned.append(prod(rows_of, halves))
            total, gap = turned[0] + turned[1], turned[0] - turned[1]
            for h in range(2):
                there = slice(h * tall, (h + 1) * tall)
                lines[m, h, near[0]] = total[there]
                lines[m, h, near[1]] = gap[there]

    @pl.when(has_above)
    def _():
        with scope("fetch"):
            down0.wait_recv()
            pl.when(has_left)(down1.wait_recv)

            @pl.when(jnp.logical_not(has_left))
            def _():
                offs[3] = jnp.zeros(offs.shape[1:], jnp.int32)

            fetched.start()
            fetched.wait()

    left_down, left_over = corner_of(corners, 1, l, side)

    per_tall = tall // OUT_ROWS
    order = [k * per_tall + i for p in range(2) for k in (p, p + 2) for i in range(per_tall)]

    def flow(src, dst, send_sem, recv_sem, device, base=0):
        return [
            piece(src, dst, chunk(order[k], OUT_ROWS), send_sem, recv_sem.at[base + k], device)
            for k in range(steps)
        ]

    rights = flow(terms, left, 10, r_left, east)
    downs = flow(lower, upper, 11, r_pool, south, base=3 * pieces if rows > 2 else 0)
    inward = flow(own, inbound, 12, r_in, inner)
    swaps = flow(own, crossed, 13, r_last, inner)
    results = flow(out, out, 14, r_last, outer)

    def rows_back(k):
        part = chunk(k, tall)
        both = []
        for which in range(2):
            here = slice(which * mid, (which + 1) * mid)
            x = [
                jnp.concatenate([lines[m, h, part, here] for h in range(2)], axis=1)
                for m in range(modes)
            ]
            both.append(after(jnp.concatenate(x, axis=0), inv, which))
        total, gap = both[0] + both[1], both[0] - both[1]
        sums = [jnp.zeros((tall, side), jnp.float32)] * 2
        for m in range(modes):
            here = slice(m * tall, (m + 1) * tall)
            new_real, new_imag = (
                jnp.concatenate(
                    [x[here, h * mid : (h + 1) * mid] for x in (total, gap)], axis=1
                )
                for h in range(2)
            )
            real, imag = (rolled[h, m, part] for h in range(2))
            sums[0] += real * new_real + imag * new_imag
            sums[1] += real * new_imag - imag * new_real
        for h in range(2):
            terms[h, part] = sums[h]

        @pl.when(has_right)
        def _():
            for j in range(steps):
                if order[j] // per_tall == k:
                    rights[j].start()

    thin_lane = lax.broadcasted_iota(jnp.int32, (OUT_ROWS, side), 1)
    thin_line = lax.broadcasted_iota(jnp.int32, (OUT_ROWS, side), 0)

    def share_out(j):
        part = chunk(order[j], OUT_ROWS)
        at = thin_line + order[j] * OUT_ROWS
        for h in range(2):
            mine = jnp.where(thin_lane >= over, terms[h, part], 0.0)
            own[h, part] = jnp.where(at >= down, mine, 0.0)
            lower[h, part] = jnp.where(at < down, mine, 0.0)

        @pl.when(has_left)
        def _():
            rights[j].wait_recv()
            for h in range(2):
                other = jnp.where(thin_lane < left_over, left[h, part], 0.0)
                own[h, part] += jnp.where(at >= left_down, other, 0.0)
                lower[h, part] += jnp.where(at < left_down, other, 0.0)

        pl.when(has_below)(downs[j].start)

    def enter(j):
        @pl.when(jnp.logical_not(has_outer))
        def _():
            if layers == 2:
                swaps[j].start()
            else:
                inward[j].start()

    def gather(j):
        part = chunk(order[j], OUT_ROWS)

        @pl.when(has_outer)
        def _():
            inward[j].wait_recv()
            for h in range(2):
                own[h, part] += inbound[h, part]
            pl.when(is_hub)(swaps[j].start)
            pl.when(jnp.logical_not(is_hub))(inward[j].start)

    def finish(j):
        part = chunk(order[j], OUT_ROWS)

        @pl.when(is_hub)
        def _():
            swaps[j].wait_recv()
            for h in range(2):
                number = own[h, part] + crossed[h, part] + DAMPING * obj[h, part]
                out[h, part] = number * weight[part]
            pl.when(has_outer)(results[j].start)

    def arrive(j):
        part = chunk(order[j], OUT_ROWS)

        @pl.when(has_above)
        def _():
            downs[j].wait_recv()
            for h in range(2):
                own[h, part] += upper[h, part]
            if j == GATE:

                @pl.when(jnp.logical_not(odd_col) & has_right)
                def _():
                    pl.semaphore_signal(
                        gate, 1, device_id=(r - 1, c + 1, l), device_id_type=pl.DeviceIdType.MESH
                    )

    begun = jnp.logical_not(has_above) & (odd_col | jnp.logical_not(has_left))

    def begin(stop):
        for s in range(stop):
            share_out(s)
            enter(s)

    for p in range(2):
        with scope(f"back{p}"):
            back(p)
        for k in (p, p + 2):
            with scope(f"rb{k}"):
                rows_back(k)
        if p == 0:
            with scope("begin"):
                pl.when(begun & odd_col)(functools.partial(begin, HEAD))
                pl.when(begun & jnp.logical_not(odd_col))(functools.partial(begin, steps // 2))

    @pl.when(is_hub)
    def _():
        with scope("weight"):
            pl.when(has_above)(functools.partial(weigh, range(4)))
            weight[...] = 1.0 / weight[...]

    def run(first, stop):
        for s in range(first, stop + LAG_IN + LAG_CROSS):
            with scope(f"out{s}"):
                if s < stop:
                    if s < (steps // 2 if first == 0 and stop == steps else HEAD):

                        @pl.when(jnp.logical_not(begun))
                        def _(s=s):
                            share_out(s)
                            arrive(s)
                            enter(s)

                    else:
                        share_out(s)
                        arrive(s)
                        enter(s)
                if first <= s - LAG_IN < stop:
                    gather(s - LAG_IN)
                if first <= s - LAG_IN - LAG_CROSS:
                    finish(s - LAG_IN - LAG_CROSS)

    pl.when(jnp.logical_not(odd_col))(functools.partial(run, 0, steps))

    @pl.when(odd_col)
    def _():
        run(0, HEAD)

        @pl.when(has_below)
        def _():
            with scope("gate"):
                pl.semaphore_wait(gate, 1)

        run(HEAD, steps)

    @pl.when(jnp.logical_not(is_hub))
    def _():
        for j in range(steps):
            with scope(f"res{j}"):
                results[j].wait_recv()
                pl.when(has_outer)(results[j].start)

    def sent(there, src, send_sem):
        @pl.when(there)
        def _():
            send(src, src, s_send.at[send_sem], r_pass.at[0], east).wait_send()

    with scope("drain"):
        part = obj.at[:, :mid]
        sent(has_left, obj, 0)
        sent(has_above, part, 1)
        sent(has_below, part, 2)
        sent(has_below & has_left & odd_col, part, 3)
        few = obj.at[:, : OVER_SIDE * IN_ROWS]
        sent(has_below & has_left & jnp.logical_not(odd_col), few, 3)
        sent(has_below & has_left & odd_col, part, 4)
        many = obj.at[:, : (2 * pieces - OVER_SIDE) * IN_ROWS]
        sent(has_above & has_right & odd_col, many, 5)
        if layers > 1:
            sent(layers > 1, offs.at[0, pl.ds(0, layers - 1)], 6)
        sent(has_right, offs.at[0], 7)
        sent(has_below, offs.at[0], 8)
        sent(has_below & has_left, offs.at[0], 9)
        sent(has_right, terms, 10)
        sent(has_below, lower, 11)
        sent(jnp.logical_not(is_hub), own, 12)
        sent(is_hub, own, 13)
        sent(has_outer, out, 14)


def tables(side):
    mid = side // 2
    steps = np.arange(mid)
    kinds = []
    for shift in range(2):
        angle = (steps[:, None] * (2 * steps[None, :] + shift) % side) * (2.0 * np.pi / side)
        real, imag = np.cos(angle) / np.sqrt(side), -np.sin(angle) / np.sqrt(side)
        kinds.append(np.block([[real, imag], [-imag, real]]))
    both = np.stack(kinds)

    def halves(x):
        x = x.astype(np.float32)
        high = x.astype(jnp.bfloat16)
        return high, (x - high.astype(np.float32)).astype(jnp.bfloat16)

    return np.stack(halves(both) + halves(both.transpose(0, 2, 1)))


def body(sizes, object_field, probe_modes, amplitudes, offsets):
    rows, cols, layers = sizes
    side = object_field.shape[1]
    assert object_field.shape[2] == side and probe_modes.shape[2] == side
    assert offsets.shape[0] == 1 and layers % 2 == 0
    assert side == PARTS * 4 * IN_ROWS and side // OUT_ROWS <= 3 * (side // IN_ROWS // 2)
    assert PARTS == 4 and side % (PARTS * OUT_ROWS) == 0
    modes = probe_modes.shape[1]
    hbm = pl.BlockSpec(memory_space=pltpu.MemorySpace.HBM)
    vmem = pl.BlockSpec(memory_space=pltpu.MemorySpace.VMEM)
    pair = (2, side, side)
    f32 = jnp.float32
    dma = pltpu.SemaphoreType.DMA
    plane = pltpu.VMEM((side, side), f32)
    whole = pltpu.VMEM(pair, f32)
    corners = (4, layers, 1, 128)
    pieces, steps = side // IN_ROWS // 2, side // OUT_ROWS
    return pl.pallas_call(
        functools.partial(kernel, sizes),
        out_shape=pltpu.VMEM(pair, f32),
        in_specs=[hbm] * 5,
        out_specs=vmem,
        scratch_shapes=[
            pltpu.SMEM((1, 2), jnp.int32),
            whole,
            pltpu.VMEM(probe_modes.shape, f32),
            pltpu.VMEM((1, side, side), f32),
        ]
        + [pltpu.VMEM((4, 2, side, side), jnp.bfloat16)]
        + [pltpu.VMEM(corners, jnp.int32), pltpu.SMEM(corners, jnp.int32)]
        + [whole] * 3
        + [
            pltpu.VMEM(probe_modes.shape, f32),
            pltpu.VMEM((modes, 2, side, side), f32),
            pltpu.VMEM((modes, 2, side, side), f32),
            pltpu.VMEM((2, modes, 2, side, side), jnp.bfloat16),
        ]
        + [plane] * 3
        + [whole] * 7
        + [dma((5,)), dma(()), dma((15,)), dma((layers - 1,)), dma((3,))]
        + [dma((pieces // 2,))] * 2
        + [dma((3 * pieces + (steps if rows > 2 else 0),))]
        + [dma((steps,))] * 3
        + [pltpu.SemaphoreType.REGULAR],
        compiler_params=pltpu.CompilerParams(
            collective_id=0, has_side_effects=True, vmem_limit_bytes=58 * 1024 * 1024
        ),
        name="update",
    )(offsets, object_field, probe_modes, amplitudes, jnp.asarray(tables(side)))


def solution(mesh):
    sizes = tuple(mesh.shape[a] for a in AXES)
    placed = (
        P(None, "row", "col"),
        P(),
        P(("row", "col", "layer"), None, None),
        P(("row", "col", "layer"), None),
    )
    return jax.shard_map(
        functools.partial(body, sizes),
        mesh=mesh,
        in_specs=placed,
        out_specs=P(None, "row", "col"),
        check_vma=False,
    )
```

```python
import contextlib
import functools

import jax
import jax.numpy as jnp
import numpy as np
from jax import lax
from jax.experimental import pallas as pl
from jax.experimental.pallas import tpu as pltpu
from jax.sharding import PartitionSpec as P

SOFTEN = 0.05
DAMPING = 0.5
AXES = ("row", "col", "layer")
PARTS = 4
IN_ROWS = 16
UNROLL = 4
OUT_ROWS = 16
LAG_IN = 6
LAG_CROSS = 7
GATE = 10
HEAD = 4
OVER_SIDE = 6


def scope(name):
    return contextlib.nullcontext()


def place():
    return tuple(lax.axis_index(a) for a in AXES)


def send(src, dst, send_sem, recv_sem, device):
    return pltpu.make_async_remote_copy(
        src_ref=src,
        dst_ref=dst,
        send_sem=send_sem,
        recv_sem=recv_sem,
        device_id=device,
        device_id_type=pl.DeviceIdType.MESH,
    )


def greet(rows, cols, layers):
    r, c, l = place()
    barrier = pltpu.get_barrier_semaphore()

    def tell(device):
        pl.semaphore_signal(
            barrier, inc=1, device_id=device, device_id_type=pl.DeviceIdType.MESH
        )

    near = (
        (c > 0, (r, c - 1, l)),
        (c < cols - 1, (r, c + 1, l)),
        (r > 0, (r - 1, c, l)),
        (r < rows - 1, (r + 1, c, l)),
        ((r > 0) & (c < cols - 1), (r - 1, c + 1, l)),
        ((r < rows - 1) & (c > 0), (r + 1, c - 1, l)),
    )
    for there, device in near:
        pl.when(there)(functools.partial(tell, device))
    for d in range(1, layers):
        tell((r, c, lax.rem(l + d, layers)))
    count = layers - 1
    for there, _ in near:
        count += there.astype(jnp.int32)
    pl.semaphore_wait(barrier, count)


def split(x):
    high = x.astype(jnp.bfloat16)
    return high, (x - high.astype(jnp.float32)).astype(jnp.bfloat16)


def prod(left, right):
    def one(a, b):
        return jnp.dot(a, b, preferred_element_type=jnp.float32)

    return one(left[0], right[0]) + (one(left[0], right[1]) + one(left[1], right[0]))


def corner_of(offs, group, layer, side):
    r, c, _ = place()
    tile_row = r - (1 if group >= 2 else 0)
    tile_col = c - (group % 2)
    return offs[group, layer, 0, 0] - tile_row * side, offs[group, layer, 0, 1] - tile_col * side


def kernel(
    sizes,
    corner_hbm, obj_hbm, probe_hbm, amp_hbm, table_hbm,
    out,
    corner, obj, probe, amp, table, offs, corners,
    right, below, diag, rolled, lines, far, parted, ratio, power, weight,
    terms, left, own, lower, upper, inbound, crossed,
    s_load, s_corner, s_send, r_off, r_pass,
    r_right, r_right2, r_pool, r_left, r_in, r_last, gate,
):
    rows, cols, layers = sizes
    side = obj.shape[1]
    mid = side // 2
    modes = probe.shape[1]
    tall = side // PARTS
    pieces = side // IN_ROWS // 2
    steps = side // OUT_ROWS
    r, c, l = place()
    has_right, has_left = c < cols - 1, c > 0
    has_below, has_above = r < rows - 1, r > 0
    half = layers // 2
    low_half = l < half
    is_hub = (l == half - 1) | (l == half)
    has_outer = (l > 0) & (l < layers - 1)
    inner = (r, c, l + jnp.where(low_half, 1, -1))
    outer = (r, c, l + jnp.where(low_half, -1, 1))
    odd = lax.rem(l, 2)
    partner = (r, c, l + 1 - 2 * odd)
    west, east = (r, c - 1, l), (r, c + 1, l)
    north, south = (r - 1, c, l), (r + 1, c, l)
    odd_col = lax.rem(c, 2) == 1

    loads = [
        pltpu.make_async_copy(src, dst, s_load.at[i])
        for i, (src, dst) in enumerate(
            (
                (corner_hbm, corner),
                (obj_hbm, obj),
                (probe_hbm, probe),
                (amp_hbm, amp),
                (table_hbm, table),
            )
        )
    ]
    for copy in loads:
        copy.start()
    with scope("greet"):
        greet(rows, cols, layers)
    with scope("load"):
        loads[1].wait()

    def chunk(k, size):
        return pl.ds(k * size, size)

    def piece(src, dst, part, send_sem, recv_sem, device):
        return send(src.at[:, part], dst.at[:, part], s_send.at[send_sem], recv_sem, device)

    lefts, lefts2, ups, shares, diags, diags2, extras, extras2 = ([] for _ in range(8))
    for i in range(pieces):
        mine, other = chunk(2 * i + odd, IN_ROWS), chunk(2 * i + 1 - odd, IN_ROWS)
        lefts.append(piece(obj, right, mine, 0, r_right.at[i // 2], west))
        lefts2.append(piece(obj, right, other, 0, r_right2.at[i // 2], west))
        ups.append(piece(obj, below, mine, 1, r_pool.at[i], north))
        shares.append(piece(below, below, mine, 2, r_pool.at[pieces + i], partner))
        diags.append(piece(below, diag, mine, 3, r_pool.at[2 * pieces + i // 2], west))
        diags2.append(piece(below, diag, other, 4, r_pool.at[2 * pieces + (pieces + i) // 2], west))
        if i >= OVER_SIDE:
            extras2.append(piece(right, diag, mine, 5, r_pool.at[2 * pieces + i // 2], north))
        extras.append(piece(right, diag, other, 5, r_pool.at[2 * pieces + (pieces + i) // 2], north))

    def two(recv_sem):
        piece(obj, right, chunk(0, 2 * IN_ROWS), 0, recv_sem, west).wait_recv()

    for copy in ups:
        pl.when(has_above)(copy.start)
    for copy in lefts2 + lefts[OVER_SIDE:] + lefts[:OVER_SIDE]:
        pl.when(has_left)(copy.start)
    with scope("load0"):
        loads[0].wait()
    at = lax.broadcasted_iota(jnp.int32, (1, 1, 128), 2)
    offs[0, pl.ds(l, 1)] = jnp.where(at == 0, corner[0, 0], corner[0, 1])
    mine = offs.at[0, pl.ds(l, 1)]
    around = [(d, lax.rem(l + d, layers)) for d in range(1, layers)]
    peers = [send(mine, mine, s_send.at[6], r_off.at[d - 1], (r, c, p)) for d, p in around]
    for peer in peers:
        peer.start()
    down = corner[0, 0] - r * side
    over = corner[0, 1] - c * side
    with scope("load2"):
        loads[2].wait()

    def prepare(m):
        for h in range(2):
            rolled[h, m] = pltpu.roll(pltpu.roll(probe[h, m], down, 0), over, 1)

    def forward(i):
        @pl.when(has_below)
        def _():
            ups[i].wait_recv()
            shares[i].start()
            pl.when(has_left & odd_col if i >= OVER_SIDE else has_left)(diags[i].start)

        if i % 2 == 0:

            @pl.when(has_above & has_right & odd_col)
            def _():
                two(r_right2.at[i // 2])
                extras[i].start()
                extras[i + 1].start()
                if i + 2 == pieces:
                    for k in range(OVER_SIDE // 2, pieces // 2):
                        two(r_right.at[k])
                    for copy in extras2:
                        copy.start()

    def forward2(i):
        @pl.when(has_below)
        def _():
            shares[i].wait_recv()
            pl.when(has_left & odd_col)(diags2[i].start)

    across = send(offs.at[0], offs.at[1], s_send.at[7], r_pass.at[0], east)
    down0 = send(offs.at[0], offs.at[2], s_send.at[8], r_pass.at[1], south)
    down1 = send(offs.at[1], offs.at[3], s_send.at[9], r_pass.at[2], south)

    def weigh(groups, first=0, last=layers):
        there = (None, has_left, has_above, has_left & has_above)
        wide = lax.broadcasted_iota(jnp.int32, (side, side), 1)
        deep = lax.broadcasted_iota(jnp.int32, (side, side), 0)
        for group in groups:

            def add(layer, carry, group=group):
                a, b = corner_of(corners, group, layer, side)
                window = pltpu.roll(pltpu.roll(power[...], a, 0), b, 1)
                keep = (deep < a) if group >= 2 else (deep >= a)
                keep &= (wide < b) if group % 2 else (wide >= b)
                weight[...] += jnp.where(keep, window, 0.0)
                return carry

            def all_layers(add=add):
                lax.fori_loop(first, last, add, 0)

            if there[group] is None:
                all_layers()
            else:
                pl.when(there[group])(all_layers)

    def fetch():
        copy = pltpu.make_async_copy(offs, corners, s_corner)
        copy.start()
        copy.wait()

    fetched = pltpu.make_async_copy(offs, corners, s_corner)

    with scope("prep"):
        for m in range(modes):
            prepare(m)
    with scope("amp"):
        power[...] = jnp.zeros_like(power)
        for m in range(modes):
            power[...] += probe[0, m] * probe[0, m] + probe[1, m] * probe[1, m]
        loads[3].wait()
        wide = lax.broadcasted_iota(jnp.int32, (side, side), 1)
        deep = lax.broadcasted_iota(jnp.int32, (side, side), 0)

        def pick(to, start):
            return to == jnp.where(start < mid, 2 * start, 2 * start - side + 1)

        turn = jnp.where(pick(wide, deep), 1.0, 0.0).astype(jnp.bfloat16)
        back_turn = jnp.where(pick(deep, wide), 1.0, 0.0).astype(jnp.bfloat16)

        def moved(x, along):
            total = None
            for _ in range(3):
                high = x.astype(jnp.bfloat16)
                x = x - high.astype(jnp.float32)
                pair = (turn, high) if along == 0 else (high, back_turn)
                one = jnp.dot(*pair, preferred_element_type=jnp.float32)
                total = one if total is None else total + one
            return total

        amp[0] = moved(moved(amp[0], 0), 1)
        weight[...] = jnp.full_like(weight, DAMPING)

    with scope("peers"):
        for peer in peers:
            peer.wait_recv()
        pl.when(has_right)(across.start)
    with scope("fwd0"):
        forward(0)
    for i in (1, 2):
        with scope(f"fwd{i}"):
            forward(i)
    with scope("across"):

        @pl.when(has_left)
        def _():
            across.wait_recv()

        @pl.when(jnp.logical_not(has_left))
        def _():
            offs[1] = jnp.zeros(offs.shape[1:], jnp.int32)

        @pl.when(has_below)
        def _():
            down0.start()
            pl.when(has_left)(down1.start)

        @pl.when(jnp.logical_not(has_above))
        def _():
            offs[2] = jnp.zeros(offs.shape[1:], jnp.int32)
            offs[3] = jnp.zeros(offs.shape[1:], jnp.int32)
            fetched.start()

    fwd, inv = (table.at[0], table.at[1]), (table.at[2], table.at[3])

    def after(x, table, which):
        return prod(split(x), (table[0][which], table[1][which]))

    def ahead(table, which, x):
        return prod((table[0][which], table[1][which]), split(x))

    lane = lax.broadcasted_iota(jnp.int32, (tall, side), 1)
    line = lax.broadcasted_iota(jnp.int32, (tall, side), 0)

    def first_part(k):
        part = chunk(k, tall)
        with scope(f"merge{k}"):
            high = line + k * tall < down
            for h in range(2):
                own[h, part] = obj[h, part]

            @pl.when(has_right & jnp.logical_not(has_above & odd_col))
            def _():
                two(r_right2.at[k])

            ready = has_above & odd_col if k >= OVER_SIDE // 2 else has_right & False
            pl.when(has_right & jnp.logical_not(ready))(lambda: two(r_right.at[k]))

            @pl.when(has_right)
            def _():
                for h in range(2):
                    own[h, part] = jnp.where(lane < over, right[h, part], own[h, part])

            @pl.when(has_below)
            def _():
                for h in range(2):
                    own[h, part] = jnp.where(high & (lane >= over), below[h, part], own[h, part])

            @pl.when(has_below & has_right)
            def _():
                two(r_pool.at[2 * pieces + k])
                two(r_pool.at[2 * pieces + pieces // 2 + k])
                for h in range(2):
                    own[h, part] = jnp.where(high & (lane < over), diag[h, part], own[h, part])

        with scope(f"first{k}"):
            patch = [own[h, part] for h in range(2)]
            sums, gaps = [], []
            for m in range(modes):
                real, imag = (rolled[h, m, part] for h in range(2))
                new = (real * patch[0] - imag * patch[1], real * patch[1] + imag * patch[0])
                sums.append(jnp.concatenate([x[:, :mid] + x[:, mid:] for x in new], axis=1))
                gaps.append(jnp.concatenate([x[:, :mid] - x[:, mid:] for x in new], axis=1))
            even = after(jnp.concatenate(sums, axis=0), fwd, 0)
            uneven = after(jnp.concatenate(gaps, axis=0), fwd, 1)
            for m in range(modes):
                here = slice(m * tall, (m + 1) * tall)
                for h in range(2):
                    there = slice(h * mid, (h + 1) * mid)
                    lines[m, h, part] = jnp.concatenate(
                        [even[here, there], uneven[here, there]], axis=1
                    )

    early = has_below & jnp.logical_not(odd_col & has_right)
    quarters = [(g, q * layers // 2, (q + 1) * layers // 2) for g in (0, 1) for q in range(2)]
    with scope("loads"):
        for copy in loads[4:]:
            copy.wait()
    for i in range(3, pieces):
        with scope(f"fwd{i}"):
            forward(i)
    for i in range(pieces):
        with scope(f"fwz{i}"):
            forward2(i)
        if i < 4:

            @pl.when(jnp.logical_not(has_above) & is_hub)
            def _(i=i):
                with scope(f"weight{i}"):
                    if i == 0:
                        fetched.wait()
                    group, start, stop = quarters[i]
                    weigh((group,), start, stop)

        if i % 2 == 1 and i > 1:
            pl.when(early)(functools.partial(first_part, i // 2 - 1))
    pl.when(early)(functools.partial(first_part, PARTS - 1))
    pl.when(jnp.logical_not(has_above | is_hub))(fetched.wait)

    @pl.when(jnp.logical_not(early))
    def _():
        for k in range(PARTS):
            first_part(k)

    ratio[...] = jnp.zeros_like(ratio)

    def columns(m, carry):
        x = [lines[m, h] for h in range(2)]
        sums = jnp.concatenate([p[:mid] + p[mid:] for p in x], axis=0)
        gaps = jnp.concatenate([p[:mid] - p[mid:] for p in x], axis=0)
        for which, y in enumerate((sums, gaps)):
            spread = ahead(inv, which, y)
            far[m, which] = spread
            here = slice(which * mid, (which + 1) * mid)
            ratio[here] += spread[:mid] * spread[:mid] + spread[mid:] * spread[mid:]
        return carry

    with scope("columns"):
        lax.fori_loop(0, modes, columns, 0, unroll=UNROLL)
    ratio[...] = amp[0] / (jnp.sqrt(ratio[...]) + SOFTEN)

    def back(p):
        near = (slice(p * tall, (p + 1) * tall), slice(mid + p * tall, mid + (p + 1) * tall))
        for m in range(modes):
            turned = []
            for which in range(2):
                if p == 0:
                    scale = ratio[which * mid : (which + 1) * mid]
                    fixed = jnp.concatenate(
                        [far[m, which, :mid] * scale, far[m, which, mid:] * scale], axis=0
                    )
                    halves = split(fixed)
                    for x in range(2):
                        parted[x, m, which] = halves[x]
                else:
                    halves = (parted[0, m, which], parted[1, m, which])
                rows_of = [
                    jnp.concatenate([t[which, here] for here in near], axis=0) for t in fwd
                ]
                turned.append(prod(rows_of, halves))
            total, gap = turned[0] + turned[1], turned[0] - turned[1]
            for h in range(2):
                there = slice(h * tall, (h + 1) * tall)
                lines[m, h, near[0]] = total[there]
                lines[m, h, near[1]] = gap[there]

    @pl.when(has_above)
    def _():
        with scope("fetch"):
            down0.wait_recv()
            pl.when(has_left)(down1.wait_recv)

            @pl.when(jnp.logical_not(has_left))
            def _():
                offs[3] = jnp.zeros(offs.shape[1:], jnp.int32)

            fetched.start()
            fetched.wait()

    left_down, left_over = corner_of(corners, 1, l, side)

    per_tall = tall // OUT_ROWS
    order = [k * per_tall + i for p in range(2) for k in (p, p + 2) for i in range(per_tall)]

    def flow(src, dst, send_sem, recv_sem, device, base=0):
        return [
            piece(src, dst, chunk(order[k], OUT_ROWS), send_sem, recv_sem.at[base + k], device)
            for k in range(steps)
        ]

    rights = flow(terms, left, 10, r_left, east)
    downs = flow(lower, upper, 11, r_pool, south, base=3 * pieces if rows > 2 else 0)
    inward = flow(own, inbound, 12, r_in, inner)
    swaps = flow(own, crossed, 13, r_last, inner)
    results = flow(out, out, 14, r_last, outer)

    def rows_back(k):
        part = chunk(k, tall)
        both = []
        for which in range(2):
            here = slice(which * mid, (which + 1) * mid)
            x = [
                jnp.concatenate([lines[m, h, part, here] for h in range(2)], axis=1)
                for m in range(modes)
            ]
            both.append(after(jnp.concatenate(x, axis=0), inv, which))
        total, gap = both[0] + both[1], both[0] - both[1]
        sums = [jnp.zeros((tall, side), jnp.float32)] * 2
        for m in range(modes):
            here = slice(m * tall, (m + 1) * tall)
            new_real, new_imag = (
                jnp.concatenate(
                    [x[here, h * mid : (h + 1) * mid] for x in (total, gap)], axis=1
                )
                for h in range(2)
            )
            real, imag = (rolled[h, m, part] for h in range(2))
            sums[0] += real * new_real + imag * new_imag
            sums[1] += real * new_imag - imag * new_real
        for h in range(2):
            terms[h, part] = sums[h]

        @pl.when(has_right)
        def _():
            for j in range(steps):
                if order[j] // per_tall == k:
                    rights[j].start()

    thin_lane = lax.broadcasted_iota(jnp.int32, (OUT_ROWS, side), 1)
    thin_line = lax.broadcasted_iota(jnp.int32, (OUT_ROWS, side), 0)

    def share_out(j):
        part = chunk(order[j], OUT_ROWS)
        at = thin_line + order[j] * OUT_ROWS
        for h in range(2):
            mine = jnp.where(thin_lane >= over, terms[h, part], 0.0)
            own[h, part] = jnp.where(at >= down, mine, 0.0)
            lower[h, part] = jnp.where(at < down, mine, 0.0)

        @pl.when(has_left)
        def _():
            rights[j].wait_recv()
            for h in range(2):
                other = jnp.where(thin_lane < left_over, left[h, part], 0.0)
                own[h, part] += jnp.where(at >= left_down, other, 0.0)
                lower[h, part] += jnp.where(at < left_down, other, 0.0)

        pl.when(has_below)(downs[j].start)

    def enter(j):
        @pl.when(jnp.logical_not(has_outer))
        def _():
            if layers == 2:
                swaps[j].start()
            else:
                inward[j].start()

    def gather(j):
        part = chunk(order[j], OUT_ROWS)

        @pl.when(has_outer)
        def _():
            inward[j].wait_recv()
            for h in range(2):
                own[h, part] += inbound[h, part]
            pl.when(is_hub)(swaps[j].start)
            pl.when(jnp.logical_not(is_hub))(inward[j].start)

    def finish(j):
        part = chunk(order[j], OUT_ROWS)

        @pl.when(is_hub)
        def _():
            swaps[j].wait_recv()
            for h in range(2):
                number = own[h, part] + crossed[h, part] + DAMPING * obj[h, part]
                out[h, part] = number * weight[part]
            pl.when(has_outer)(results[j].start)

    def arrive(j):
        part = chunk(order[j], OUT_ROWS)

        @pl.when(has_above)
        def _():
            downs[j].wait_recv()
            for h in range(2):
                own[h, part] += upper[h, part]
            if j == GATE:

                @pl.when(jnp.logical_not(odd_col) & has_right)
                def _():
                    pl.semaphore_signal(
                        gate, 1, device_id=(r - 1, c + 1, l), device_id_type=pl.DeviceIdType.MESH
                    )

    begun = jnp.logical_not(has_above) & (odd_col | jnp.logical_not(has_left))

    def begin(stop):
        for s in range(stop):
            share_out(s)
            enter(s)

    for p in range(2):
        with scope(f"back{p}"):
            back(p)
        for k in (p, p + 2):
            with scope(f"rb{k}"):
                rows_back(k)
        if p == 0:
            with scope("begin"):
                pl.when(begun & odd_col)(functools.partial(begin, HEAD))
                pl.when(begun & jnp.logical_not(odd_col))(functools.partial(begin, steps // 2))

    @pl.when(is_hub)
    def _():
        with scope("weight"):
            pl.when(has_above)(functools.partial(weigh, range(4)))
            weight[...] = 1.0 / weight[...]

    def run(first, stop):
        for s in range(first, stop + LAG_IN + LAG_CROSS):
            with scope(f"out{s}"):
                if s < stop:
                    if s < (steps // 2 if first == 0 and stop == steps else HEAD):

                        @pl.when(jnp.logical_not(begun))
                        def _(s=s):
                            share_out(s)
                            arrive(s)
                            enter(s)

                    else:
                        share_out(s)
                        arrive(s)
                        enter(s)
                if first <= s - LAG_IN < stop:
                    gather(s - LAG_IN)
                if first <= s - LAG_IN - LAG_CROSS:
                    finish(s - LAG_IN - LAG_CROSS)

    pl.when(jnp.logical_not(odd_col))(functools.partial(run, 0, steps))

    @pl.when(odd_col)
    def _():
        run(0, HEAD)

        @pl.when(has_below)
        def _():
            with scope("gate"):
                pl.semaphore_wait(gate, 1)

        run(HEAD, steps)

    @pl.when(jnp.logical_not(is_hub))
    def _():
        for j in range(steps):
            with scope(f"res{j}"):
                results[j].wait_recv()
                pl.when(has_outer)(results[j].start)

    def sent(there, src, send_sem):
        @pl.when(there)
        def _():
            send(src, src, s_send.at[send_sem], r_pass.at[0], east).wait_send()

    with scope("drain"):
        part = obj.at[:, :mid]
        sent(has_left, obj, 0)
        sent(has_above, part, 1)
        sent(has_below, part, 2)
        sent(has_below & has_left & odd_col, part, 3)
        few = obj.at[:, : OVER_SIDE * IN_ROWS]
        sent(has_below & has_left & jnp.logical_not(odd_col), few, 3)
        sent(has_below & has_left & odd_col, part, 4)
        many = obj.at[:, : (2 * pieces - OVER_SIDE) * IN_ROWS]
        sent(has_above & has_right & odd_col, many, 5)
        if layers > 1:
            sent(layers > 1, offs.at[0, pl.ds(0, layers - 1)], 6)
        sent(has_right, offs.at[0], 7)
        sent(has_below, offs.at[0], 8)
        sent(has_below & has_left, offs.at[0], 9)
        sent(has_right, terms, 10)
        sent(has_below, lower, 11)
        sent(jnp.logical_not(is_hub), own, 12)
        sent(is_hub, own, 13)
        sent(has_outer, out, 14)


def tables(side):
    mid = side // 2
    steps = np.arange(mid)
    kinds = []
    for shift in range(2):
        angle = (steps[:, None] * (2 * steps[None, :] + shift) % side) * (2.0 * np.pi / side)
        real, imag = np.cos(angle) / np.sqrt(side), -np.sin(angle) / np.sqrt(side)
        kinds.append(np.block([[real, imag], [-imag, real]]))
    both = np.stack(kinds)

    def halves(x):
        x = x.astype(np.float32)
        high = x.astype(jnp.bfloat16)
        return high, (x - high.astype(np.float32)).astype(jnp.bfloat16)

    return np.stack(halves(both) + halves(both.transpose(0, 2, 1)))


def body(sizes, object_field, probe_modes, amplitudes, offsets):
    rows, cols, layers = sizes
    side = object_field.shape[1]
    assert object_field.shape[2] == side and probe_modes.shape[2] == side
    assert offsets.shape[0] == 1 and layers % 2 == 0
    assert side == PARTS * 4 * IN_ROWS and side // OUT_ROWS <= 3 * (side // IN_ROWS // 2)
    assert PARTS == 4 and side % (PARTS * OUT_ROWS) == 0
    modes = probe_modes.shape[1]
    hbm = pl.BlockSpec(memory_space=pltpu.MemorySpace.HBM)
    vmem = pl.BlockSpec(memory_space=pltpu.MemorySpace.VMEM)
    pair = (2, side, side)
    f32 = jnp.float32
    dma = pltpu.SemaphoreType.DMA
    plane = pltpu.VMEM((side, side), f32)
    whole = pltpu.VMEM(pair, f32)
    corners = (4, layers, 1, 128)
    pieces, steps = side // IN_ROWS // 2, side // OUT_ROWS
    return pl.pallas_call(
        functools.partial(kernel, sizes),
        out_shape=pltpu.VMEM(pair, f32),
        in_specs=[hbm] * 5,
        out_specs=vmem,
        scratch_shapes=[
            pltpu.SMEM((1, 2), jnp.int32),
            whole,
            pltpu.VMEM(probe_modes.shape, f32),
            pltpu.VMEM((1, side, side), f32),
        ]
        + [pltpu.VMEM((4, 2, side, side), jnp.bfloat16)]
        + [pltpu.VMEM(corners, jnp.int32), pltpu.SMEM(corners, jnp.int32)]
        + [whole] * 3
        + [
            pltpu.VMEM(probe_modes.shape, f32),
            pltpu.VMEM((modes, 2, side, side), f32),
            pltpu.VMEM((modes, 2, side, side), f32),
            pltpu.VMEM((2, modes, 2, side, side), jnp.bfloat16),
        ]
        + [plane] * 3
        + [whole] * 7
        + [dma((5,)), dma(()), dma((15,)), dma((layers - 1,)), dma((3,))]
        + [dma((pieces // 2,))] * 2
        + [dma((3 * pieces + (steps if rows > 2 else 0),))]
        + [dma((steps,))] * 3
        + [pltpu.SemaphoreType.REGULAR],
        compiler_params=pltpu.CompilerParams(
            collective_id=0, has_side_effects=True, vmem_limit_bytes=58 * 1024 * 1024
        ),
        name="update",
    )(offsets, object_field, probe_modes, amplitudes, jnp.asarray(tables(side)))


def solution(mesh):
    sizes = tuple(mesh.shape[a] for a in AXES)
    placed = (
        P(None, "row", "col"),
        P(),
        P(("row", "col", "layer"), None, None),
        P(("row", "col", "layer"), None),
    )
    return jax.shard_map(
        functools.partial(body, sizes),
        mesh=mesh,
        in_specs=placed,
        out_specs=P(None, "row", "col"),
        check_vma=False,
    )
```

```python
import contextlib
import functools

import jax
import jax.numpy as jnp
import numpy as np
from jax import lax
from jax.experimental import pallas as pl
from jax.experimental.pallas import tpu as pltpu
from jax.sharding import PartitionSpec as P

SOFTEN = 0.05
DAMPING = 0.5
AXES = ("row", "col", "layer")
PARTS = 4
IN_ROWS = 16
UNROLL = 4
OUT_ROWS = 16
EVEN_LAGS = (6, 8)
ODD_LAGS = (5, 7)
GATE = 10
HEAD = 4
OVER_SIDE = 6


def scope(name):
    return contextlib.nullcontext()


def place():
    return tuple(lax.axis_index(a) for a in AXES)


def send(src, dst, send_sem, recv_sem, device):
    return pltpu.make_async_remote_copy(
        src_ref=src,
        dst_ref=dst,
        send_sem=send_sem,
        recv_sem=recv_sem,
        device_id=device,
        device_id_type=pl.DeviceIdType.MESH,
    )


def greet(rows, cols, layers):
    r, c, l = place()
    barrier = pltpu.get_barrier_semaphore()

    def tell(device):
        pl.semaphore_signal(
            barrier, inc=1, device_id=device, device_id_type=pl.DeviceIdType.MESH
        )

    near = (
        (c > 0, (r, c - 1, l)),
        (c < cols - 1, (r, c + 1, l)),
        (r > 0, (r - 1, c, l)),
        (r < rows - 1, (r + 1, c, l)),
        ((r > 0) & (c < cols - 1), (r - 1, c + 1, l)),
        ((r < rows - 1) & (c > 0), (r + 1, c - 1, l)),
    )
    for there, device in near:
        pl.when(there)(functools.partial(tell, device))
    for d in range(1, layers):
        tell((r, c, lax.rem(l + d, layers)))
    count = layers - 1
    for there, _ in near:
        count += there.astype(jnp.int32)
    pl.semaphore_wait(barrier, count)


def split(x):
    high = x.astype(jnp.bfloat16)
    return high, (x - high.astype(jnp.float32)).astype(jnp.bfloat16)


def prod(left, right):
    def one(a, b):
        return jnp.dot(a, b, preferred_element_type=jnp.float32)

    return one(left[0], right[0]) + (one(left[0], right[1]) + one(left[1], right[0]))


def corner_of(offs, group, layer, side):
    r, c, _ = place()
    tile_row = r - (1 if group >= 2 else 0)
    tile_col = c - (group % 2)
    return offs[group, layer, 0, 0] - tile_row * side, offs[group, layer, 0, 1] - tile_col * side


def kernel(
    sizes,
    corner_hbm, obj_hbm, probe_hbm, amp_hbm, table_hbm,
    out,
    corner, obj, probe, amp, table, offs, corners,
    right, below, diag, rolled, lines, far, parted, ratio, power, weight,
    terms, left, own, lower, upper, inbound, crossed,
    s_load, s_corner, s_send, r_off, r_pass,
    r_right, r_right2, r_pool, r_left, r_in, r_last, gate,
):
    rows, cols, layers = sizes
    side = obj.shape[1]
    mid = side // 2
    modes = probe.shape[1]
    tall = side // PARTS
    pieces = side // IN_ROWS // 2
    steps = side // OUT_ROWS
    r, c, l = place()
    has_right, has_left = c < cols - 1, c > 0
    has_below, has_above = r < rows - 1, r > 0
    half = layers // 2
    low_half = l < half
    is_hub = (l == half - 1) | (l == half)
    has_outer = (l > 0) & (l < layers - 1)
    inner = (r, c, l + jnp.where(low_half, 1, -1))
    outer = (r, c, l + jnp.where(low_half, -1, 1))
    odd = lax.rem(l, 2)
    partner = (r, c, l + 1 - 2 * odd)
    west, east = (r, c - 1, l), (r, c + 1, l)
    north, south = (r - 1, c, l), (r + 1, c, l)
    odd_col = lax.rem(c, 2) == 1

    loads = [
        pltpu.make_async_copy(src, dst, s_load.at[i])
        for i, (src, dst) in enumerate(
            (
                (corner_hbm, corner),
                (obj_hbm, obj),
                (probe_hbm, probe),
                (amp_hbm, amp),
                (table_hbm, table),
            )
        )
    ]
    for copy in loads:
        copy.start()
    with scope("greet"):
        greet(rows, cols, layers)
    with scope("load"):
        loads[1].wait()

    def chunk(k, size):
        return pl.ds(k * size, size)

    def piece(src, dst, part, send_sem, recv_sem, device):
        return send(src.at[:, part], dst.at[:, part], s_send.at[send_sem], recv_sem, device)

    lefts, lefts2, ups, shares, diags, diags2, extras, extras2 = ([] for _ in range(8))
    for i in range(pieces):
        mine, other = chunk(2 * i + odd, IN_ROWS), chunk(2 * i + 1 - odd, IN_ROWS)
        lefts.append(piece(obj, right, mine, 0, r_right.at[i // 2], west))
        lefts2.append(piece(obj, right, other, 0, r_right2.at[i // 2], west))
        ups.append(piece(obj, below, mine, 1, r_pool.at[i], north))
        shares.append(piece(below, below, mine, 2, r_pool.at[pieces + i], partner))
        diags.append(piece(below, diag, mine, 3, r_pool.at[2 * pieces + i // 2], west))
        diags2.append(piece(below, diag, other, 4, r_pool.at[2 * pieces + (pieces + i) // 2], west))
        if i >= OVER_SIDE:
            extras2.append(piece(right, diag, mine, 5, r_pool.at[2 * pieces + i // 2], north))
        extras.append(piece(right, diag, other, 5, r_pool.at[2 * pieces + (pieces + i) // 2], north))

    def two(recv_sem):
        piece(obj, right, chunk(0, 2 * IN_ROWS), 0, recv_sem, west).wait_recv()

    for copy in ups:
        pl.when(has_above)(copy.start)
    for copy in lefts2 + lefts[OVER_SIDE:] + lefts[:OVER_SIDE]:
        pl.when(has_left)(copy.start)
    with scope("load0"):
        loads[0].wait()
    at = lax.broadcasted_iota(jnp.int32, (1, 1, 128), 2)
    offs[0, pl.ds(l, 1)] = jnp.where(at == 0, corner[0, 0], corner[0, 1])
    mine = offs.at[0, pl.ds(l, 1)]
    around = [(d, lax.rem(l + d, layers)) for d in range(1, layers)]
    peers = [send(mine, mine, s_send.at[6], r_off.at[d - 1], (r, c, p)) for d, p in around]
    for peer in peers:
        peer.start()
    down = corner[0, 0] - r * side
    over = corner[0, 1] - c * side
    with scope("load2"):
        loads[2].wait()

    def prepare(m):
        for h in range(2):
            rolled[h, m] = pltpu.roll(pltpu.roll(probe[h, m], down, 0), over, 1)

    def forward(i):
        @pl.when(has_below)
        def _():
            ups[i].wait_recv()
            shares[i].start()
            pl.when(has_left & odd_col if i >= OVER_SIDE else has_left)(diags[i].start)

        if i % 2 == 0:

            @pl.when(has_above & has_right & odd_col)
            def _():
                two(r_right2.at[i // 2])
                extras[i].start()
                extras[i + 1].start()
                if i + 2 == pieces:
                    for k in range(OVER_SIDE // 2, pieces // 2):
                        two(r_right.at[k])
                    for copy in extras2:
                        copy.start()

    def forward2(i):
        @pl.when(has_below)
        def _():
            shares[i].wait_recv()
            pl.when(has_left & odd_col)(diags2[i].start)

    across = send(offs.at[0], offs.at[1], s_send.at[7], r_pass.at[0], east)
    down0 = send(offs.at[0], offs.at[2], s_send.at[8], r_pass.at[1], south)
    down1 = send(offs.at[1], offs.at[3], s_send.at[9], r_pass.at[2], south)

    def weigh(groups, first=0, last=layers):
        there = (None, has_left, has_above, has_left & has_above)
        wide = lax.broadcasted_iota(jnp.int32, (side, side), 1)
        deep = lax.broadcasted_iota(jnp.int32, (side, side), 0)
        for group in groups:

            def add(layer, carry, group=group):
                a, b = corner_of(corners, group, layer, side)
                window = pltpu.roll(pltpu.roll(power[...], a, 0), b, 1)
                keep = (deep < a) if group >= 2 else (deep >= a)
                keep &= (wide < b) if group % 2 else (wide >= b)
                weight[...] += jnp.where(keep, window, 0.0)
                return carry

            def all_layers(add=add):
                lax.fori_loop(first, last, add, 0)

            if there[group] is None:
                all_layers()
            else:
                pl.when(there[group])(all_layers)

    def fetch():
        copy = pltpu.make_async_copy(offs, corners, s_corner)
        copy.start()
        copy.wait()

    fetched = pltpu.make_async_copy(offs, corners, s_corner)

    with scope("prep"):
        for m in range(modes):
            prepare(m)
    with scope("amp"):
        power[...] = jnp.zeros_like(power)
        for m in range(modes):
            power[...] += probe[0, m] * probe[0, m] + probe[1, m] * probe[1, m]
        loads[3].wait()
        wide = lax.broadcasted_iota(jnp.int32, (side, side), 1)
        deep = lax.broadcasted_iota(jnp.int32, (side, side), 0)

        def pick(to, start):
            return to == jnp.where(start < mid, 2 * start, 2 * start - side + 1)

        turn = jnp.where(pick(wide, deep), 1.0, 0.0).astype(jnp.bfloat16)
        back_turn = jnp.where(pick(deep, wide), 1.0, 0.0).astype(jnp.bfloat16)

        def moved(x, along):
            total = None
            for _ in range(3):
                high = x.astype(jnp.bfloat16)
                x = x - high.astype(jnp.float32)
                pair = (turn, high) if along == 0 else (high, back_turn)
                one = jnp.dot(*pair, preferred_element_type=jnp.float32)
                total = one if total is None else total + one
            return total

        amp[0] = moved(moved(amp[0], 0), 1)
        weight[...] = jnp.full_like(weight, DAMPING)

    with scope("peers"):
        for peer in peers:
            peer.wait_recv()
        pl.when(has_right)(across.start)
    with scope("fwd0"):
        forward(0)
    for i in (1, 2):
        with scope(f"fwd{i}"):
            forward(i)
    with scope("across"):

        @pl.when(has_left)
        def _():
            across.wait_recv()

        @pl.when(jnp.logical_not(has_left))
        def _():
            offs[1] = jnp.zeros(offs.shape[1:], jnp.int32)

        @pl.when(has_below)
        def _():
            down0.start()
            pl.when(has_left)(down1.start)

        @pl.when(jnp.logical_not(has_above))
        def _():
            offs[2] = jnp.zeros(offs.shape[1:], jnp.int32)
            offs[3] = jnp.zeros(offs.shape[1:], jnp.int32)
            fetched.start()

    fwd, inv = (table.at[0], table.at[1]), (table.at[2], table.at[3])

    def after(x, table, which):
        return prod(split(x), (table[0][which], table[1][which]))

    def ahead(table, which, x):
        return prod((table[0][which], table[1][which]), split(x))

    lane = lax.broadcasted_iota(jnp.int32, (tall, side), 1)
    line = lax.broadcasted_iota(jnp.int32, (tall, side), 0)

    def first_part(k):
        part = chunk(k, tall)
        with scope(f"merge{k}"):
            high = line + k * tall < down
            for h in range(2):
                own[h, part] = obj[h, part]

            @pl.when(has_right & jnp.logical_not(has_above & odd_col))
            def _():
                two(r_right2.at[k])

            ready = has_above & odd_col if k >= OVER_SIDE // 2 else has_right & False
            pl.when(has_right & jnp.logical_not(ready))(lambda: two(r_right.at[k]))

            @pl.when(has_right)
            def _():
                for h in range(2):
                    own[h, part] = jnp.where(lane < over, right[h, part], own[h, part])

            @pl.when(has_below)
            def _():
                for h in range(2):
                    own[h, part] = jnp.where(high & (lane >= over), below[h, part], own[h, part])

            @pl.when(has_below & has_right)
            def _():
                two(r_pool.at[2 * pieces + k])
                two(r_pool.at[2 * pieces + pieces // 2 + k])
                for h in range(2):
                    own[h, part] = jnp.where(high & (lane < over), diag[h, part], own[h, part])

        with scope(f"first{k}"):
            patch = [own[h, part] for h in range(2)]
            sums, gaps = [], []
            for m in range(modes):
                real, imag = (rolled[h, m, part] for h in range(2))
                new = (real * patch[0] - imag * patch[1], real * patch[1] + imag * patch[0])
                sums.append(jnp.concatenate([x[:, :mid] + x[:, mid:] for x in new], axis=1))
                gaps.append(jnp.concatenate([x[:, :mid] - x[:, mid:] for x in new], axis=1))
            even = after(jnp.concatenate(sums, axis=0), fwd, 0)
            uneven = after(jnp.concatenate(gaps, axis=0), fwd, 1)
            for m in range(modes):
                here = slice(m * tall, (m + 1) * tall)
                for h in range(2):
                    there = slice(h * mid, (h + 1) * mid)
                    lines[m, h, part] = jnp.concatenate(
                        [even[here, there], uneven[here, there]], axis=1
                    )

    early = has_below & jnp.logical_not(odd_col & has_right)
    quarters = [(g, q * layers // 2, (q + 1) * layers // 2) for g in (0, 1) for q in range(2)]
    with scope("loads"):
        for copy in loads[4:]:
            copy.wait()
    for i in range(3, pieces):
        with scope(f"fwd{i}"):
            forward(i)
    for i in range(pieces):
        with scope(f"fwz{i}"):
            forward2(i)
        if i < 4:

            @pl.when(jnp.logical_not(has_above) & is_hub)
            def _(i=i):
                with scope(f"weight{i}"):
                    if i == 0:
                        fetched.wait()
                    group, start, stop = quarters[i]
                    weigh((group,), start, stop)

        if i % 2 == 1 and i > 1:
            pl.when(early)(functools.partial(first_part, i // 2 - 1))
    pl.when(early)(functools.partial(first_part, PARTS - 1))
    pl.when(jnp.logical_not(has_above | is_hub))(fetched.wait)

    @pl.when(jnp.logical_not(early))
    def _():
        for k in range(PARTS):
            first_part(k)

    ratio[...] = jnp.zeros_like(ratio)

    def columns(m, carry):
        x = [lines[m, h] for h in range(2)]
        sums = jnp.concatenate([p[:mid] + p[mid:] for p in x], axis=0)
        gaps = jnp.concatenate([p[:mid] - p[mid:] for p in x], axis=0)
        for which, y in enumerate((sums, gaps)):
            spread = ahead(inv, which, y)
            far[m, which] = spread
            here = slice(which * mid, (which + 1) * mid)
            ratio[here] += spread[:mid] * spread[:mid] + spread[mid:] * spread[mid:]
        return carry

    with scope("columns"):
        lax.fori_loop(0, modes, columns, 0, unroll=UNROLL)
    ratio[...] = amp[0] / (jnp.sqrt(ratio[...]) + SOFTEN)

    def back(p):
        near = (slice(p * tall, (p + 1) * tall), slice(mid + p * tall, mid + (p + 1) * tall))
        for m in range(modes):
            turned = []
            for which in range(2):
                if p == 0:
                    scale = ratio[which * mid : (which + 1) * mid]
                    fixed = jnp.concatenate(
                        [far[m, which, :mid] * scale, far[m, which, mid:] * scale], axis=0
                    )
                    halves = split(fixed)
                    for x in range(2):
                        parted[x, m, which] = halves[x]
                else:
                    halves = (parted[0, m, which], parted[1, m, which])
                rows_of = [
                    jnp.concatenate([t[which, here] for here in near], axis=0) for t in fwd
                ]
                turned.append(prod(rows_of, halves))
            total, gap = turned[0] + turned[1], turned[0] - turned[1]
            for h in range(2):
                there = slice(h * tall, (h + 1) * tall)
                lines[m, h, near[0]] = total[there]
                lines[m, h, near[1]] = gap[there]

    @pl.when(has_above)
    def _():
        with scope("fetch"):
            down0.wait_recv()
            pl.when(has_left)(down1.wait_recv)

            @pl.when(jnp.logical_not(has_left))
            def _():
                offs[3] = jnp.zeros(offs.shape[1:], jnp.int32)

            fetched.start()
            fetched.wait()

    left_down, left_over = corner_of(corners, 1, l, side)

    per_tall = tall // OUT_ROWS
    order = [k * per_tall + i for p in range(2) for k in (p, p + 2) for i in range(per_tall)]

    def flow(src, dst, send_sem, recv_sem, device, base=0):
        return [
            piece(src, dst, chunk(order[k], OUT_ROWS), send_sem, recv_sem.at[base + k], device)
            for k in range(steps)
        ]

    rights = flow(terms, left, 10, r_left, east)
    downs = flow(lower, upper, 11, r_pool, south, base=3 * pieces if rows > 2 else 0)
    inward = flow(own, inbound, 12, r_in, inner)
    swaps = flow(own, crossed, 13, r_last, inner)
    results = flow(out, out, 14, r_last, outer)

    def rows_back(k):
        part = chunk(k, tall)
        both = []
        for which in range(2):
            here = slice(which * mid, (which + 1) * mid)
            x = [
                jnp.concatenate([lines[m, h, part, here] for h in range(2)], axis=1)
                for m in range(modes)
            ]
            both.append(after(jnp.concatenate(x, axis=0), inv, which))
        total, gap = both[0] + both[1], both[0] - both[1]
        sums = [jnp.zeros((tall, side), jnp.float32)] * 2
        for m in range(modes):
            here = slice(m * tall, (m + 1) * tall)
            new_real, new_imag = (
                jnp.concatenate(
                    [x[here, h * mid : (h + 1) * mid] for x in (total, gap)], axis=1
                )
                for h in range(2)
            )
            real, imag = (rolled[h, m, part] for h in range(2))
            sums[0] += real * new_real + imag * new_imag
            sums[1] += real * new_imag - imag * new_real
        for h in range(2):
            terms[h, part] = sums[h]

        @pl.when(has_right)
        def _():
            for j in range(steps):
                if order[j] // per_tall == k:
                    rights[j].start()

    thin_lane = lax.broadcasted_iota(jnp.int32, (OUT_ROWS, side), 1)
    thin_line = lax.broadcasted_iota(jnp.int32, (OUT_ROWS, side), 0)

    def share_out(j):
        part = chunk(order[j], OUT_ROWS)
        at = thin_line + order[j] * OUT_ROWS
        for h in range(2):
            mine = jnp.where(thin_lane >= over, terms[h, part], 0.0)
            own[h, part] = jnp.where(at >= down, mine, 0.0)
            lower[h, part] = jnp.where(at < down, mine, 0.0)

        @pl.when(has_left)
        def _():
            rights[j].wait_recv()
            for h in range(2):
                other = jnp.where(thin_lane < left_over, left[h, part], 0.0)
                own[h, part] += jnp.where(at >= left_down, other, 0.0)
                lower[h, part] += jnp.where(at < left_down, other, 0.0)

        pl.when(has_below)(downs[j].start)

    def enter(j):
        @pl.when(jnp.logical_not(has_outer))
        def _():
            if layers == 2:
                swaps[j].start()
            else:
                inward[j].start()

    def gather(j):
        part = chunk(order[j], OUT_ROWS)

        @pl.when(has_outer)
        def _():
            inward[j].wait_recv()
            for h in range(2):
                own[h, part] += inbound[h, part]
            pl.when(is_hub)(swaps[j].start)
            pl.when(jnp.logical_not(is_hub))(inward[j].start)

    def finish(j):
        part = chunk(order[j], OUT_ROWS)

        @pl.when(is_hub)
        def _():
            swaps[j].wait_recv()
            for h in range(2):
                number = own[h, part] + crossed[h, part] + DAMPING * obj[h, part]
                out[h, part] = number * weight[part]
            pl.when(has_outer)(results[j].start)

    def arrive(j):
        part = chunk(order[j], OUT_ROWS)

        @pl.when(has_above)
        def _():
            downs[j].wait_recv()
            for h in range(2):
                own[h, part] += upper[h, part]
            if j == GATE:

                @pl.when(jnp.logical_not(odd_col) & has_right)
                def _():
                    pl.semaphore_signal(
                        gate, 1, device_id=(r - 1, c + 1, l), device_id_type=pl.DeviceIdType.MESH
                    )

    begun = jnp.logical_not(has_above) & (odd_col | jnp.logical_not(has_left))

    def begin(stop):
        for s in range(stop):
            share_out(s)
            enter(s)

    for p in range(2):
        with scope(f"back{p}"):
            back(p)
        for k in (p, p + 2):
            with scope(f"rb{k}"):
                rows_back(k)
        if p == 0:
            with scope("begin"):
                pl.when(begun & odd_col)(functools.partial(begin, HEAD))
                pl.when(begun & jnp.logical_not(odd_col))(functools.partial(begin, steps // 2))

    @pl.when(is_hub)
    def _():
        with scope("weight"):
            pl.when(has_above)(functools.partial(weigh, range(4)))
            weight[...] = 1.0 / weight[...]

    def run(first, stop, lags):
        lag_in, lag_cross = lags
        for s in range(first, stop + lag_in + lag_cross):
            with scope(f"out{s}"):
                if s < stop:
                    if s < (steps // 2 if first == 0 and stop == steps else HEAD):

                        @pl.when(jnp.logical_not(begun))
                        def _(s=s):
                            share_out(s)
                            arrive(s)
                            enter(s)

                    else:
                        share_out(s)
                        arrive(s)
                        enter(s)
                if first <= s - lag_in < stop:
                    gather(s - lag_in)
                if first <= s - lag_in - lag_cross:
                    finish(s - lag_in - lag_cross)

    pl.when(jnp.logical_not(odd_col))(functools.partial(run, 0, steps, EVEN_LAGS))

    @pl.when(odd_col)
    def _():
        run(0, HEAD, ODD_LAGS)

        @pl.when(has_below)
        def _():
            with scope("gate"):
                pl.semaphore_wait(gate, 1)

        run(HEAD, steps, ODD_LAGS)

    @pl.when(jnp.logical_not(is_hub))
    def _():
        for j in range(steps):
            with scope(f"res{j}"):
                results[j].wait_recv()
                pl.when(has_outer)(results[j].start)

    def sent(there, src, send_sem):
        @pl.when(there)
        def _():
            send(src, src, s_send.at[send_sem], r_pass.at[0], east).wait_send()

    with scope("drain"):
        part = obj.at[:, :mid]
        sent(has_left, obj, 0)
        sent(has_above, part, 1)
        sent(has_below, part, 2)
        sent(has_below & has_left & odd_col, part, 3)
        few = obj.at[:, : OVER_SIDE * IN_ROWS]
        sent(has_below & has_left & jnp.logical_not(odd_col), few, 3)
        sent(has_below & has_left & odd_col, part, 4)
        many = obj.at[:, : (2 * pieces - OVER_SIDE) * IN_ROWS]
        sent(has_above & has_right & odd_col, many, 5)
        if layers > 1:
            sent(layers > 1, offs.at[0, pl.ds(0, layers - 1)], 6)
        sent(has_right, offs.at[0], 7)
        sent(has_below, offs.at[0], 8)
        sent(has_below & has_left, offs.at[0], 9)
        sent(has_right, terms, 10)
        sent(has_below, lower, 11)
        sent(jnp.logical_not(is_hub), own, 12)
        sent(is_hub, own, 13)
        sent(has_outer, out, 14)


def tables(side):
    mid = side // 2
    steps = np.arange(mid)
    kinds = []
    for shift in range(2):
        angle = (steps[:, None] * (2 * steps[None, :] + shift) % side) * (2.0 * np.pi / side)
        real, imag = np.cos(angle) / np.sqrt(side), -np.sin(angle) / np.sqrt(side)
        kinds.append(np.block([[real, imag], [-imag, real]]))
    both = np.stack(kinds)

    def halves(x):
        x = x.astype(np.float32)
        high = x.astype(jnp.bfloat16)
        return high, (x - high.astype(np.float32)).astype(jnp.bfloat16)

    return np.stack(halves(both) + halves(both.transpose(0, 2, 1)))


def body(sizes, object_field, probe_modes, amplitudes, offsets):
    rows, cols, layers = sizes
    side = object_field.shape[1]
    assert object_field.shape[2] == side and probe_modes.shape[2] == side
    assert offsets.shape[0] == 1 and layers % 2 == 0
    assert side == PARTS * 4 * IN_ROWS and side // OUT_ROWS <= 3 * (side // IN_ROWS // 2)
    assert PARTS == 4 and side % (PARTS * OUT_ROWS) == 0
    modes = probe_modes.shape[1]
    hbm = pl.BlockSpec(memory_space=pltpu.MemorySpace.HBM)
    vmem = pl.BlockSpec(memory_space=pltpu.MemorySpace.VMEM)
    pair = (2, side, side)
    f32 = jnp.float32
    dma = pltpu.SemaphoreType.DMA
    plane = pltpu.VMEM((side, side), f32)
    whole = pltpu.VMEM(pair, f32)
    corners = (4, layers, 1, 128)
    pieces, steps = side // IN_ROWS // 2, side // OUT_ROWS
    return pl.pallas_call(
        functools.partial(kernel, sizes),
        out_shape=pltpu.VMEM(pair, f32),
        in_specs=[hbm] * 5,
        out_specs=vmem,
        scratch_shapes=[
            pltpu.SMEM((1, 2), jnp.int32),
            whole,
            pltpu.VMEM(probe_modes.shape, f32),
            pltpu.VMEM((1, side, side), f32),
        ]
        + [pltpu.VMEM((4, 2, side, side), jnp.bfloat16)]
        + [pltpu.VMEM(corners, jnp.int32), pltpu.SMEM(corners, jnp.int32)]
        + [whole] * 3
        + [
            pltpu.VMEM(probe_modes.shape, f32),
            pltpu.VMEM((modes, 2, side, side), f32),
            pltpu.VMEM((modes, 2, side, side), f32),
            pltpu.VMEM((2, modes, 2, side, side), jnp.bfloat16),
        ]
        + [plane] * 3
        + [whole] * 7
        + [dma((5,)), dma(()), dma((15,)), dma((layers - 1,)), dma((3,))]
        + [dma((pieces // 2,))] * 2
        + [dma((3 * pieces + (steps if rows > 2 else 0),))]
        + [dma((steps,))] * 3
        + [pltpu.SemaphoreType.REGULAR],
        compiler_params=pltpu.CompilerParams(
            collective_id=0, has_side_effects=True, vmem_limit_bytes=58 * 1024 * 1024
        ),
        name="update",
    )(offsets, object_field, probe_modes, amplitudes, jnp.asarray(tables(side)))


def solution(mesh):
    sizes = tuple(mesh.shape[a] for a in AXES)
    placed = (
        P(None, "row", "col"),
        P(),
        P(("row", "col", "layer"), None, None),
        P(("row", "col", "layer"), None),
    )
    return jax.shard_map(
        functools.partial(body, sizes),
        mesh=mesh,
        in_specs=placed,
        out_specs=P(None, "row", "col"),
        check_vma=False,
    )
```
